32 devices in a mesh: img: 32 (over z, y, x, core).
Axes of the slice: x: 2, y: 2, z: 4, core: 2. Of those that a mesh axis runs over, the one named last changes fastest.
Arguments:
- queries: bfloat16 [12288, 1024], P('img'), may hold values from -10 to 10
- keys: bfloat16 [12288, 1024], P('img'), may hold values from -10 to 10
- values: bfloat16 [12288, 1024], P('img'), may hold values from -6 to 6
- out_grad: bfloat16 [12288, 1024], P('img'), may hold values from -6 to 6
- image_ids: int32 [12288], P('img'), may hold values from 0 to 31, never falling along the last dimension, each value on 1 to 1152 neighbouring positions
Outputs:
- attended: bfloat16 [12288, 1024], P('img')
- query_grad: bfloat16 [12288, 1024], P('img')
- key_grad: bfloat16 [12288, 1024], P('img')
- value_grad: bfloat16 [12288, 1024], P('img')
The draws below stay inside these ranges and needn't reach their ends.
Inputs may be any that keep to these rules, and one draw needn't show every extreme that they name: `image_ids`: the regions of one image stand in consecutive rows, and ids rise along the rows; an image has 1 to 1152 regions, and some image has exactly 1152.
All inputs are finite; a program needn't handle non-finite values.
Results may differ from the reference program's by a relative error of at most 0.0069.
Values may be sent and summed in bfloat16 or wider, within the bound.
A program may use at most 192 MiB of HBM per device.

```python
import math
import jax
import jax.numpy as jnp
import numpy as np
from jax import lax

D = 1024
HEADS = 16
ROWS_DEV = 384
REACH = 3
MOST = 1152
TOKENS = 12288
N_IMG = 32


def paired_features(key):
    base = jax.random.fold_in(key, 7)
    first, second = jax.random.split(base, 2)
    shape = (TOKENS, D)
    query_f = jnp.clip(jax.random.normal(first, shape, jnp.float32), -6.0, 6.0)
    key_f = jnp.clip(jax.random.normal(second, shape, jnp.float32), -6.0, 6.0)
    return (query_f, key_f)


def draw_queries(key, part):
    return paired_features(key)[0].astype(jnp.bfloat16)


def draw_keys(key, part):
    return paired_features(key)[1].astype(jnp.bfloat16)


def levels(key, extent, cuts, least, top_value):
    gain = 1.0
    for axis_at, shards_of in cuts:
        steps = jax.random.uniform(jax.random.fold_in(jax.random.fold_in(key, 6), axis_at), (shards_of,), jnp.float32, least / len(cuts), top_value / len(cuts))
        gain = gain * jnp.repeat(jnp.exp(steps), extent[axis_at] // shards_of).reshape((-1,) + (1,) * (len(extent) - 1 - axis_at))
    return gain


def profile(amount, total, limit, lean):
    portions = [(1 << 20) // math.isqrt(rank ** lean) + 1 for rank in range(2, amount + 1)]
    spare, holding = total - limit - (amount - 1), [1] * (amount - 1)
    while spare > 0:
        free = [i for i in range(amount - 1) if holding[i] < limit]
        pool, remaining = sum([portions[i] for i in free]), spare
        for i in free:
            more = min(limit - holding[i], max(1, remaining * portions[i] // pool), spare)
            holding[i] = holding[i] + more
            spare = spare - more
    return np.array([limit] + holding)


def ragged_sizes(own_key, amount, total, limit, lean):
    if amount == 2:
        one = jax.random.randint(own_key, (), max(1, total - limit), min(limit, total - 1) + 1)
        return jnp.stack([one, total - one])
    tallies = jnp.asarray(profile(amount, total, limit, lean), jnp.int32)
    twos = (amount - 1) // 2
    donor, taker = tallies[1:1 + 2 * twos:2], tallies[2:2 + 2 * twos:2]
    room = jnp.minimum(donor - 1, limit - taker)
    shifted = jax.random.randint(jax.random.fold_in(own_key, 1), (twos,), 0, 1 << 20) % (room + 1)
    tallies = tallies.at[1:1 + 2 * twos:2].set(donor - shifted).at[2:2 + 2 * twos:2].set(taker + shifted)
    return tallies[jax.random.permutation(jax.random.fold_in(own_key, 2), amount)]


def bell_draw(own_key, dims, spread, reach, cuts=(), held_as=jnp.bfloat16):
    drawn = spread * jax.random.normal(own_key, dims, jnp.float32)
    if cuts:
        drawn = drawn * levels(own_key, dims, cuts, -0.22, 0.18)
    return jnp.clip(drawn, -reach, reach).astype(held_as)


def setup_inputs(seed: int = 0) -> dict:
    arg_keys = jax.random.split(jax.random.key(seed), 6)
    return {
        "queries": draw_queries(jax.random.fold_in(arg_keys[5], 71), 0),
        "keys": draw_keys(jax.random.fold_in(arg_keys[5], 71), 0),
        "values": bell_draw(arg_keys[2], (TOKENS, D), 1.0, 6.0, ((0, 32),)),
        "out_grad": bell_draw(arg_keys[3], (TOKENS, D), 1.0, 6.0, ((0, 32),)),
        "image_ids": jnp.searchsorted(jnp.cumsum(ragged_sizes(arg_keys[4], N_IMG, TOKENS, MOST, 1)), jnp.arange(TOKENS), side="right").astype(jnp.int32),
    }


def attend_block(query_rows, key_rows, value_rows, grad_rows, query_tags, key_tags):
    row_count = query_rows.shape[0]
    width = key_rows.shape[0]
    head_dim = D // HEADS
    score_scale = 1.0 / math.sqrt(head_dim)
    query_f = query_rows.astype(jnp.float32).reshape(row_count, HEADS, head_dim)
    key_f = key_rows.astype(jnp.float32).reshape(width, HEADS, head_dim)
    value_f = value_rows.astype(jnp.float32).reshape(width, HEADS, head_dim)
    grad_f = grad_rows.astype(jnp.float32).reshape(row_count, HEADS, head_dim)
    same_image = query_tags[:, None] == key_tags[None, :]
    scores = jnp.einsum('rhd,whd->hrw', query_f, key_f) * score_scale
    scores = jnp.where(same_image[None], scores, -1e+30)
    peak = lax.optimization_barrier(jnp.max(scores, axis=-1, keepdims=True))
    weights = jnp.exp(scores - peak)
    probs = weights / lax.optimization_barrier(jnp.sum(weights, axis=-1, keepdims=True))
    probs_b = lax.optimization_barrier(probs.astype(jnp.bfloat16)).astype(jnp.float32)
    attended = jnp.einsum('hrw,whd->rhd', probs_b, value_f).reshape(row_count, D).astype(jnp.bfloat16)
    dprobs = jnp.einsum('rhd,whd->hrw', grad_f, value_f)
    row_delta = lax.optimization_barrier(jnp.sum(probs * dprobs, axis=-1, keepdims=True))
    dscores = probs * (dprobs - row_delta)
    dscores_b = lax.optimization_barrier(dscores.astype(jnp.bfloat16)).astype(jnp.float32)
    query_grad = (jnp.einsum('hrw,whd->rhd', dscores_b, key_f) * score_scale).reshape(row_count, D).astype(jnp.bfloat16)
    key_grad = (jnp.einsum('hrw,rhd->whd', dscores_b, query_f) * score_scale).reshape(width, D)
    value_grad = jnp.einsum('hrw,rhd->whd', probs_b, grad_f).reshape(width, D)
    return (attended, query_grad, key_grad, value_grad)

def reference(queries, keys, values, out_grad, image_ids):
    row_count = ROWS_DEV
    width = (2 * REACH + 1) * row_count
    margin = REACH * row_count
    image_tags = (image_ids + 1).astype(jnp.int32)
    keys_padded = jnp.pad(keys, ((margin, margin), (0, 0)))
    values_padded = jnp.pad(values, ((margin, margin), (0, 0)))
    tags_padded = jnp.pad(image_tags, (margin, margin))
    start_acc = (jnp.zeros((TOKENS + 2 * margin, D), jnp.float32), jnp.zeros((TOKENS + 2 * margin, D), jnp.float32))

    def one_block(carry, block):
        key_acc, value_acc = carry
        start = (block * row_count).astype(jnp.int32)
        query_rows = lax.dynamic_slice_in_dim(queries, start, row_count, 0)
        grad_rows = lax.dynamic_slice_in_dim(out_grad, start, row_count, 0)
        query_tags = lax.dynamic_slice_in_dim(image_tags, start, row_count, 0)
        key_rows = lax.dynamic_slice_in_dim(keys_padded, start, width, 0)
        value_rows = lax.dynamic_slice_in_dim(values_padded, start, width, 0)
        key_tags = lax.dynamic_slice_in_dim(tags_padded, start, width, 0)
        attended, query_grad, key_grad, value_grad = attend_block(query_rows, key_rows, value_rows, grad_rows, query_tags, key_tags)
        key_acc = lax.dynamic_update_slice_in_dim(key_acc, lax.dynamic_slice_in_dim(key_acc, start, width, 0) + key_grad, start, 0)
        value_acc = lax.dynamic_update_slice_in_dim(value_acc, lax.dynamic_slice_in_dim(value_acc, start, width, 0) + value_grad, start, 0)
        return ((key_acc, value_acc), (attended, query_grad))
    (key_acc, value_acc), (attended, query_grad) = lax.scan(one_block, start_acc, jnp.arange(N_IMG, dtype=jnp.int32))
    attended = attended.reshape(TOKENS, D)
    query_grad = query_grad.reshape(TOKENS, D)
    key_grad = key_acc[margin:margin + TOKENS].astype(jnp.bfloat16)
    value_grad = value_acc[margin:margin + TOKENS].astype(jnp.bfloat16)
    return (attended, query_grad, key_grad, value_grad)
```

```python
import math

import jax
import jax.numpy as jnp
from jax import lax
from jax.experimental import pallas as pl
from jax.experimental.pallas import tpu as pltpu
from jax.sharding import PartitionSpec as P

HEAD_DIM = 64
REACH = 3
LANES = 128
TAG_ROWS = 16
TQ = 256
TK = 256
OUTSIDE = -1e30
VMEM = pl.BlockSpec(memory_space=pltpu.VMEM)


def dot_nt(a, b):
    return lax.dot_general(a, b, (((1,), (1,)), ((), ())), preferred_element_type=jnp.float32)


def dot_nn(a, b):
    return lax.dot_general(a, b, (((1,), (0,)), ((), ())), preferred_element_type=jnp.float32)


def call(kernel, name, outs, scratch, flops, *args):
    return pl.pallas_call(
        kernel,
        name=name,
        out_shape=tuple(outs),
        in_specs=[VMEM] * len(args),
        out_specs=(VMEM,) * len(outs),
        scratch_shapes=scratch,
        compiler_params=pltpu.CompilerParams(vmem_limit_bytes=48 * 1024 * 1024),
        cost_estimate=pl.CostEstimate(flops=flops, bytes_accessed=4_000_000, transcendentals=0),
    )(*args)


def bf16(*shape):
    return jax.ShapeDtypeStruct(shape, jnp.bfloat16)


def low_lanes(rows):
    return lax.broadcasted_iota(jnp.int32, (rows, LANES), 1) < HEAD_DIM


def swap(x):
    return pltpu.roll(x, HEAD_DIM, 1)


def mate_at(step, team):
    return lax.rem(lax.rem(lax.axis_index("img"), team) + step, team)


def pack(team, q, k, v, g, tags):
    rows = q.shape[0]

    def kernel(q_ref, k_ref, v_ref, g_ref, tag_ref, *outs):
        low = low_lanes(rows)
        scale = 1.0 / math.sqrt(HEAD_DIM)
        for step in range(team):
            lanes = pl.ds(pl.multiple_of(mate_at(step, team) * LANES, LANES), LANES)
            qx = q_ref[:, lanes].astype(jnp.float32) * scale
            gx = g_ref[:, lanes].astype(jnp.float32)
            kx = k_ref[:, lanes].astype(jnp.float32)
            vx = v_ref[:, lanes].astype(jnp.float32)
            kv0, qg0, kv1, qg1 = outs[step * 4 : step * 4 + 4]
            kv0[:rows, :] = jnp.where(low, kx, swap(vx)).astype(jnp.bfloat16)
            qg0[...] = jnp.where(low, qx, swap(gx)).astype(jnp.bfloat16)
            kv1[...] = jnp.where(low, swap(kx), vx).astype(jnp.bfloat16)
            qg1[...] = jnp.where(low, swap(qx), gx).astype(jnp.bfloat16)
            kv0[rows:, :] = tag_ref[...]

    one = (bf16(rows + TAG_ROWS, LANES), bf16(rows, LANES), bf16(rows, LANES), bf16(rows, LANES))
    outs = call(kernel, "pack", one * team, [], 1_000_000, q, k, v, g, tags)
    return [outs[i::4] for i in range(4)]


def exchange(pieces, count, team):
    got = [pieces[0]]
    for step in range(1, team):
        perm = [(base + i, base + (i + step) % team)
                for base in range(0, count, team) for i in range(team)]
        got.append(lax.ppermute(pieces[step], "img", perm))
    return got


def shift(x, count, by):
    return lax.ppermute(x, "img", [(i, i + by) for i in range(count) if 0 <= i + by < count])


def assemble(team, pieces):
    block = pieces[0].shape[0]
    near = REACH * block

    def kernel(*refs):
        ins, (whole, first, last) = refs[:team], refs[team:]
        for step, src in enumerate(ins):
            mate = mate_at(team - step, team)
            whole[pl.ds(pl.multiple_of(mate * block, 16), block), :] = src[...]
        first[...] = whole[:near, :]
        last[...] = whole[(team - REACH) * block :, :]

    outs = (bf16(team * block, LANES), bf16(near, LANES), bf16(near, LANES))
    return call(kernel, "assemble", outs, [], 100_000, *pieces)


def attend_kernel(team, rows, own_tags, chunk_block, *refs):
    (kv_own, kv_before, kv_after, tags_in, *qg_in), refs = refs[: 4 + team], refs[4 + team :]
    outs, (dkv_own, part_before, part_after), refs = refs[:team], refs[team : team + 3], refs[team + 3 :]
    kvo, kvt, qg, s_buf, dp_buf, dkv, begins, ends, dqatt, acc = refs
    halo = REACH * rows
    own = team * rows
    span = own + 2 * halo
    width = chunk_block
    scale = 1.0 / math.sqrt(HEAD_DIM)
    low = low_lanes(TQ)

    for i in range(REACH):
        kvo[i * rows : (i + 1) * rows, :LANES] = kv_before[i * width : i * width + rows, :]
        kvo[halo + own + i * rows : halo + own + (i + 1) * rows, :LANES] = (
            kv_after[i * width : i * width + rows, :])
    for i in range(team):
        kvo[halo + i * rows : halo + (i + 1) * rows, :LANES] = (
            kv_own[i * width : i * width + rows, :])
        mate = mate_at(team - i, team)
        qg[pl.ds(pl.multiple_of(mate * rows, 16), rows), :] = qg_in[i][...]

    def marks(i, c):
        at = pl.ds(pl.multiple_of(i * LANES, LANES), LANES)
        tag = tags_in[pl.ds(i, 1), :]
        ids = lax.broadcasted_iota(jnp.int32, (LANES, LANES), 0).astype(jnp.float32)
        inside = (tag > 0.0) & (tag < 1e8)
        slot = tag - jnp.floor(tag * (1.0 / LANES)) * LANES
        mark = jnp.where((ids == slot) | ~inside, 1.0, 0.0)
        kvo[at, LANES:] = mark.T.astype(jnp.bfloat16)
        kvt[:, at] = kvo[at, :LANES].astype(jnp.float32).T.astype(jnp.bfloat16)
        return c

    lax.fori_loop(0, span // LANES, marks, 0)
    tiles = own // TQ
    for tile in range(tiles):
        row = (halo + tile * TQ) // LANES
        tags = tags_in[...]
        first = tags_in[row : row + 1, :1]
        final = tags_in[row + TQ // LANES - 1 : row + TQ // LANES, LANES - 1 :]
        begins[tile] = jnp.sum((tags < first).astype(jnp.int32))
        ends[tile] = jnp.sum((tags <= final).astype(jnp.int32))

    dkv[...] = jnp.zeros_like(dkv)

    def one_tile(tile, carry):
        row0 = pl.multiple_of(tile * TQ, TQ)
        rows_here = pl.ds(row0, TQ)
        key0 = (begins[tile] // LANES) * LANES
        steps = (ends[tile] - key0 + TK - 1) // TK
        key0 = jnp.minimum(key0, span - steps * TK)
        x = qg[rows_here, :]
        mark = kvo[pl.ds(pl.multiple_of(halo + row0, LANES), TQ), LANES:].astype(jnp.float32)
        apart = jnp.where(mark > 0.5, 0.0, OUTSIDE).astype(jnp.bfloat16)
        zero = jnp.zeros_like(x)
        q1 = jnp.where(low, x, zero)
        g1 = jnp.where(low, zero, x)
        q2 = jnp.concatenate([q1, apart], 1)
        gq = jnp.concatenate([q1, g1], 0)

        def score_step(j, peak):
            keys = pl.ds(pl.multiple_of(key0 + j * TK, LANES), TK)
            held = pl.ds(pl.multiple_of(j * TK, TK), TK)
            s = dot_nt(kvo[keys, :], q2)
            s_buf[held, :] = s
            dp_buf[held, :] = dot_nt(kvo[keys, :LANES], g1)
            return jnp.maximum(peak, jnp.max(s.reshape(TK // 8, 8, TQ), 0))

        peak = lax.fori_loop(0, steps, score_step, jnp.full((8, TQ), -3e38, jnp.float32))
        peak = jnp.max(peak, 0, keepdims=True)

        def weight_step(j, sums):
            total, delta = sums
            held = pl.ds(pl.multiple_of(j * TK, TK), TK)
            w = jnp.exp(s_buf[held, :] - peak)
            s_buf[held, :] = w
            wd = w * dp_buf[held, :]
            total = total + jnp.sum(w.reshape(TK // 8, 8, TQ), 0)
            delta = delta + jnp.sum(wd.reshape(TK // 8, 8, TQ), 0)
            return total, delta

        nothing = jnp.zeros((8, TQ), jnp.float32)
        total, delta = lax.fori_loop(0, steps, weight_step, (nothing, nothing))
        inverse = 1.0 / jnp.sum(total, 0, keepdims=True)
        delta = jnp.sum(delta, 0, keepdims=True) * inverse
        acc[...] = jnp.zeros_like(acc)

        def grad_step(j, c):
            keys = pl.ds(pl.multiple_of(key0 + j * TK, LANES), TK)
            held = pl.ds(pl.multiple_of(j * TK, TK), TK)
            p = s_buf[held, :] * inverse
            ds = (p * (dp_buf[held, :] - delta)).astype(jnp.bfloat16)
            p = p.astype(jnp.bfloat16)
            acc[:HEAD_DIM, :] += dot_nn(kvt[:HEAD_DIM, keys], ds)
            acc[HEAD_DIM:, :] += dot_nn(kvt[HEAD_DIM:, keys], p)
            dkv[keys, :] += dot_nn(jnp.concatenate([ds, p], 1), gq)
            return c

        lax.fori_loop(0, steps, grad_step, 0)
        both = acc[...].T
        dqatt[rows_here, :] = jnp.where(low, both * scale, both).astype(jnp.bfloat16)
        return carry

    lax.fori_loop(0, tiles, one_tile, 0)
    for step, out in enumerate(outs):
        mate = mate_at(step, team)
        out[...] = dqatt[pl.ds(pl.multiple_of(mate * rows, 16), rows), :]
    part_before[...] = dkv[:halo, :].astype(jnp.bfloat16)
    part_after[...] = dkv[halo + own :, :].astype(jnp.bfloat16)
    dkv_own[...] = dkv[halo : halo + own, :]


def attend(team, rows, kv_own, kv_before, kv_after, tags, qg):
    halo = REACH * rows
    own = team * rows
    span = own + 2 * halo
    width = kv_own.shape[0] // team
    held = -(-min(2 * halo + TQ + LANES + TK, span + TK) // TK) * TK
    outs = (bf16(rows, LANES),) * team + (
        jax.ShapeDtypeStruct((own, LANES), jnp.float32), bf16(halo, LANES), bf16(halo, LANES))
    scratch = [
        pltpu.VMEM((span, 2 * LANES), jnp.bfloat16),
        pltpu.VMEM((LANES, span), jnp.bfloat16),
        pltpu.VMEM((own, LANES), jnp.bfloat16),
        pltpu.VMEM((held, TQ), jnp.float32),
        pltpu.VMEM((held, TQ), jnp.float32),
        pltpu.VMEM((span, LANES), jnp.float32),
        pltpu.SMEM((own // TQ,), jnp.int32),
        pltpu.SMEM((own // TQ,), jnp.int32),
        pltpu.VMEM((own, LANES), jnp.bfloat16),
        pltpu.VMEM((LANES, TQ), jnp.float32),
    ]
    outs = call(lambda *refs: attend_kernel(team, rows, None, width, *refs), "attend", outs, scratch,
                30_000_000_000, kv_own, kv_before, kv_after, tags, *qg)
    return outs[:team], outs[team:]


def combine(team, rows, dkv, from_above, from_below):
    def kernel(own_ref, above_ref, below_ref, *outs):
        for step, out in enumerate(outs):
            mate = mate_at(step, team)
            total = own_ref[pl.ds(pl.multiple_of(mate * rows, 16), rows), :]
            high = pl.multiple_of(jnp.maximum(mate - (team - REACH), 0) * rows, 16)
            down = pl.multiple_of(jnp.minimum(mate, REACH - 1) * rows, 16)
            a = above_ref[pl.ds(high, rows), :].astype(jnp.float32)
            b = below_ref[pl.ds(down, rows), :].astype(jnp.float32)
            total = total + jnp.where(mate >= team - REACH, a, 0.0)
            total = total + jnp.where(mate < REACH, b, 0.0)
            out[...] = total.astype(jnp.bfloat16)

    return call(kernel, "combine", (bf16(rows, LANES),) * team, [], 1_000_000,
                dkv, from_above, from_below)


def unpack(team, first, second, name):
    rows = first[0].shape[0]

    def kernel(*refs):
        one, two, (left, right) = refs[:team], refs[team : 2 * team], refs[2 * team :]
        low = low_lanes(rows)
        for step in range(team):
            lanes = pl.ds(pl.multiple_of(mate_at(team - step, team) * LANES, LANES), LANES)
            a = one[step][...].astype(jnp.float32)
            b = two[step][...].astype(jnp.float32)
            left[:, lanes] = jnp.where(low, a, swap(b)).astype(jnp.bfloat16)
            right[:, lanes] = jnp.where(low, swap(a), b).astype(jnp.bfloat16)

    return call(kernel, name, (bf16(rows, team * LANES),) * 2, [], 1_000_000, *first, *second)


def window_tags(team, rows, own, before, after):
    block = rows + TAG_ROWS

    def of(x, blocks):
        return jnp.concatenate(
            [x[i * block + rows : i * block + rows + rows // LANES] for i in range(blocks)], 0
        ).astype(jnp.float32)

    late = of(after, REACH)
    return jnp.concatenate(
        [of(before, REACH), of(own, team), jnp.where(late == 0.0, 1e9, late)], 0)


def shards(queries, keys, values, out_grad, image_ids):
    rows, features = queries.shape
    count = lax.axis_size("img")
    team = features // LANES
    tags = jnp.pad((image_ids + 1).reshape(rows // LANES, LANES).astype(jnp.bfloat16),
                   ((0, TAG_ROWS - rows // LANES), (0, 0)))
    kv0, qg0, kv1, qg1 = pack(team, queries, keys, values, out_grad, tags)
    kv0 = exchange(kv0, count, team)
    qg0 = exchange(qg0, count, team)
    kv1 = exchange(kv1, count, team)
    qg1 = exchange(qg1, count, team)
    done = []
    tags = None
    for kv, qg in ((kv0, qg0), (kv1, qg1)):
        own, first, last = assemble(team, kv)
        before = shift(last, count, team)
        after = shift(first, count, -team)
        if tags is None:
            tags = window_tags(team, rows, own, before, after)
        dqatt, (dkv, part_before, part_after) = attend(team, rows, own, before, after, tags, qg)
        dqatt = exchange(dqatt, count, team)
        from_above = shift(part_before, count, -team)
        from_below = shift(part_after, count, team)
        done.append((dqatt, exchange(combine(team, rows, dkv, from_above, from_below), count, team)))
    query_grad, attended = unpack(team, done[0][0], done[1][0], "unpack_queries")
    key_grad, value_grad = unpack(team, done[0][1], done[1][1], "unpack_keys")
    return attended, query_grad, key_grad, value_grad


def solution(mesh):
    in_specs = (P("img", None), P("img", None), P("img", None), P("img", None), P("img"))
    out_specs = (P("img", None), P("img", None), P("img", None), P("img", None))
    return jax.shard_map(shards, mesh=mesh, in_specs=in_specs, out_specs=out_specs, check_vma=False)
```

```python
import math

import jax
import jax.numpy as jnp
from jax import lax
from jax.experimental import pallas as pl
from jax.experimental.pallas import tpu as pltpu
from jax.sharding import PartitionSpec as P

HEAD_DIM = 64
REACH = 3
LANES = 128
TAG_ROWS = 8
TQ = 256
TK = 256
SB = 64
NO_TAG = 1 << 30
OUTSIDE = -1e30
MESH = pl.DeviceIdType.MESH
VMEM = pl.BlockSpec(memory_space=pltpu.VMEM)
ANY = pl.BlockSpec(memory_space=pl.ANY)
HBM = pl.BlockSpec(memory_space=pltpu.HBM)


def dot_nt(a, b):
    return lax.dot_general(a, b, (((1,), (1,)), ((), ())), preferred_element_type=jnp.float32)


def dot_nn(a, b):
    return lax.dot_general(a, b, (((1,), (0,)), ((), ())), preferred_element_type=jnp.float32)


def bf16(*shape):
    return jax.ShapeDtypeStruct(shape, jnp.bfloat16)


def f32(*shape):
    return jax.ShapeDtypeStruct(shape, jnp.float32)


def greet(base, pos, team, up, down):
    barrier = pltpu.get_barrier_semaphore()
    for step in range(1, team):
        mate = base + lax.rem(pos + step, team)
        pl.semaphore_signal(barrier, inc=1, device_id=(mate,), device_id_type=MESH)
    pl.semaphore_signal(barrier, inc=1, device_id=(up,), device_id_type=MESH)
    pl.semaphore_signal(barrier, inc=1, device_id=(down,), device_id_type=MESH)
    pl.semaphore_wait(barrier, team + 1)


def place(count, team):
    me = lax.axis_index("img")
    pos = lax.rem(me, team)
    return me, me - pos, pos, lax.rem(me + team, count), lax.rem(me + count - team, count)


def remote(src, dst, send_sem, recv_sem, device):
    return pltpu.make_async_remote_copy(
        src_ref=src, dst_ref=dst, send_sem=send_sem, recv_sem=recv_sem,
        device_id=(device,), device_id_type=MESH)


def lanes_of(pos):
    return pl.ds(pl.multiple_of(pos * LANES, LANES), LANES)


def gather_kernel(count, team, *refs):
    ins, outs = refs[:5], refs[5:10]
    kt, vt, qt, marks = refs[10:14]
    send, recv, halo_send, halo_recv, local = refs[14:]
    tags, kw, vw, _, _ = outs
    me, base, pos, up, down = place(count, team)
    above = me + team < count
    below = me >= team
    greet(base, pos, team, up, down)
    rows = [src.shape[0] for src in ins]
    halos = [REACH * r if t < 3 else 0 for t, r in enumerate(rows)]
    copies, own = [], []
    for t, (src, dst) in enumerate(zip(ins, outs)):
        mine = pl.ds(pl.multiple_of(halos[t] + pos * rows[t], 8), rows[t])
        for step in range(1, team):
            mate = lax.rem(pos + step, team)
            part = src if t == 0 else src.at[:, lanes_of(mate)]
            copy = remote(part, dst.at[mine, :], send.at[t, step], recv.at[t, step], base + mate)
            copy.start()
            copies.append(copy)
        part = src if t == 0 else src.at[:, lanes_of(pos)]
        copy = pltpu.make_async_copy(part, dst.at[mine, :], local.at[t])
        copy.start()
        own.append(copy)

    def halo_copies(t):
        dst, r, h = outs[t], rows[t], halos[t]
        down_copy = remote(dst.at[pl.ds(h, h), :], dst.at[pl.ds(h + team * r, h), :],
                           halo_send.at[t, 0], halo_recv.at[t, 0], down)
        up_copy = remote(dst.at[pl.ds(team * r, h), :], dst.at[pl.ds(0, h), :],
                         halo_send.at[t, 1], halo_recv.at[t, 1], up)
        return down_copy, up_copy

    def arrived(t):
        for copy in copies[t * (team - 1) : (t + 1) * (team - 1)]:
            copy.wait_recv()
        own[t].wait()

    def forward(t):
        down_copy, up_copy = halo_copies(t)
        pl.when(below)(down_copy.start)
        pl.when(above)(up_copy.start)

    def halo_arrived(t):
        down_copy, up_copy = halo_copies(t)
        pl.when(above)(down_copy.wait_recv)
        pl.when(below)(up_copy.wait_recv)

    def flip(src, dst, start, size):
        def step(i, c):
            for u in range(3):
                at = pl.ds(pl.multiple_of(start + (3 * i + u) * LANES, LANES), LANES)
                dst[:, at] = src[at, :].astype(jnp.float32).T.astype(jnp.bfloat16)
            return c
        lax.fori_loop(0, size // LANES // 3, step, 0)

    span = kw.shape[0]
    halo = halos[1]
    inner = span - 2 * halo

    @pl.when(jnp.logical_not(below))
    def _():
        kw[:halo, :] = jnp.zeros((halo, LANES), jnp.bfloat16)
        vw[:halo, :] = jnp.zeros((halo, LANES), jnp.bfloat16)
        used = lax.rem(lax.broadcasted_iota(jnp.int32, (halos[0], LANES), 0), TAG_ROWS)
        tags[: halos[0], :] = jnp.where(used < rows[1] // LANES, 0, NO_TAG)

    @pl.when(jnp.logical_not(above))
    def _():
        kw[halo + inner :, :] = jnp.zeros((halo, LANES), jnp.bfloat16)
        vw[halo + inner :, :] = jnp.zeros((halo, LANES), jnp.bfloat16)
        tags[halos[0] + team * rows[0] :, :] = jnp.full((halos[0], LANES), NO_TAG, jnp.int32)

    arrived(0)
    forward(0)
    arrived(1)
    forward(1)
    halo_arrived(0)
    ids = lax.broadcasted_iota(jnp.int32, (LANES, LANES), 0)

    def mark(i, c):
        for u in range(rows[1] // LANES):
            at = pl.ds(pl.multiple_of(i * rows[1] + u * LANES, LANES), LANES)
            tag = tags[pl.ds(i * TAG_ROWS + u, 1), :]
            outside = (tag <= 0) | (tag >= NO_TAG)
            hit = jnp.where((ids == lax.rem(tag, LANES)) | outside, 1.0, 0.0)
            marks[at, :] = hit.T.astype(jnp.bfloat16)
        return c

    lax.fori_loop(0, span // rows[1], mark, 0)
    flip(kw, kt, halo, inner)
    arrived(2)
    forward(2)
    halo_arrived(1)
    flip(kw, kt, 0, halo)
    flip(kw, kt, halo + inner, halo)
    flip(vw, vt, halo, inner)
    arrived(3)
    flip(outs[3], qt, 0, inner)
    halo_arrived(2)
    flip(vw, vt, 0, halo)
    flip(vw, vt, halo + inner, halo)
    arrived(4)
    for t in range(3):
        down_copy, up_copy = halo_copies(t)
        pl.when(below)(down_copy.wait_send)
        pl.when(above)(up_copy.wait_send)
    for copy in copies:
        copy.wait_send()


def gather(count, team, tags, arrays):
    rows = arrays[0].shape[0]
    span = (team + 2 * REACH) * rows
    return pl.pallas_call(
        lambda *refs: gather_kernel(count, team, *refs),
        out_shape=(
            jax.ShapeDtypeStruct(((team + 2 * REACH) * TAG_ROWS, LANES), jnp.int32),
            bf16(span, LANES), bf16(span, LANES), bf16(team * rows, LANES), bf16(team * rows, LANES),
            bf16(LANES, span), bf16(LANES, span), bf16(LANES, team * rows), bf16(span, LANES)),
        in_specs=[VMEM] + [HBM] * 4,
        out_specs=(VMEM,) * 9,
        scratch_shapes=[
            pltpu.SemaphoreType.DMA((5, team)),
            pltpu.SemaphoreType.DMA((5, team)),
            pltpu.SemaphoreType.DMA((3, 2)),
            pltpu.SemaphoreType.DMA((3, 2)),
            pltpu.SemaphoreType.DMA((5,)),
        ],
        compiler_params=pltpu.CompilerParams(
            collective_id=0, has_side_effects=True, vmem_limit_bytes=16 * 1024 * 1024),
        name="gather",
    )(tags, *arrays)


def attend_kernel(team, rows, *refs):
    tags, kw, vw, qw, gw, kt, vt, qt, marks = refs[:9]
    att_ref, dq_ref, dk_own, dv_own, dk_before, dk_after, dv_before, dv_after = refs[9:17]
    (s_buf, dp_buf, w_buf, p_buf, ds_buf, tops, sums, deltas, dk, dv, att_acc, dq_acc,
     qs, gs, qd, begins, ends) = refs[17:]
    halo = REACH * rows
    own = team * rows
    span = own + 2 * halo
    scale = 1.0 / math.sqrt(HEAD_DIM)
    low = lax.broadcasted_iota(jnp.int32, (TQ, LANES), 1) < HEAD_DIM
    ids = lax.broadcasted_iota(jnp.int32, (LANES, LANES), 0)
    tiles = own // TQ

    def tag_row(row):
        return (row // rows + REACH) * TAG_ROWS + row % rows // LANES

    for tile in range(tiles):
        first = tags[tag_row(tile * TQ) : tag_row(tile * TQ) + 1, :1]
        at = tag_row(tile * TQ + TQ - 1)
        final = tags[at : at + 1, LANES - 1 :]
        every = tags[...]
        begins[tile] = jnp.sum((every < first).astype(jnp.int32))
        ends[tile] = jnp.sum((every <= final).astype(jnp.int32))

    dk[...] = jnp.zeros_like(dk)
    dv[...] = jnp.zeros_like(dv)

    def one_tile(tile, carry):
        row0 = pl.multiple_of(tile * TQ, TQ)
        rows_here = pl.ds(row0, TQ)
        key0 = (begins[tile] // LANES) * LANES
        steps = (ends[tile] - key0 + TK - 1) // TK
        key0 = jnp.minimum(key0, span - steps * TK)

        q = qw[rows_here, :].astype(jnp.float32) * scale
        g = gw[rows_here, :].astype(jnp.float32)
        qd[:TQ, :] = jnp.where(low, q, 0.0).astype(jnp.bfloat16)
        qd[TQ:, :] = jnp.where(low, 0.0, q).astype(jnp.bfloat16)
        gs[:TQ, :] = jnp.where(low, g, 0.0).astype(jnp.bfloat16)
        gs[TQ:, :] = jnp.where(low, 0.0, g).astype(jnp.bfloat16)
        across = (qt[:, rows_here].astype(jnp.float32) * scale).astype(jnp.bfloat16)
        nothing = jnp.zeros((HEAD_DIM, TQ), jnp.bfloat16)
        qs[:HEAD_DIM, :TQ] = across[:HEAD_DIM]
        qs[HEAD_DIM:LANES, :TQ] = nothing
        qs[:HEAD_DIM, TQ:] = nothing
        qs[HEAD_DIM:LANES, TQ:] = across[HEAD_DIM:]
        for u in range(TQ // LANES):
            strip = tile * (TQ // LANES) + u
            per = rows // LANES
            tag = tags[pl.ds((strip // per + REACH) * TAG_ROWS + lax.rem(strip, per), 1), :]
            apart = jnp.where(ids == lax.rem(tag, LANES), 0.0, OUTSIDE).astype(jnp.bfloat16)
            qs[LANES:, u * LANES : (u + 1) * LANES] = apart
            qs[LANES:, TQ + u * LANES : TQ + (u + 1) * LANES] = apart

        def at_keys(j):
            return pl.ds(pl.multiple_of(key0 + j * TK, LANES), TK)

        def held(j):
            return pl.ds(pl.multiple_of(j * TK, TK), TK)

        def scores(j):
            keys = at_keys(j)
            s_buf[held(j), :] = dot_nn(jnp.concatenate([kw[keys, :], marks[keys, :]], 1), qs[...])
            dp_buf[held(j), :] = dot_nt(vw[keys, :], gs[...])

        def weights(j, top):
            for b in range(TK // SB):
                here = pl.ds(pl.multiple_of(j * TK + b * SB, SB), SB)
                at = pl.ds(pl.multiple_of((j * (TK // SB) + b) * 8, 8), 8)
                s = s_buf[here, :].reshape(SB // 8, 8, 2 * TQ)
                most = jnp.max(s, 0)
                w = jnp.exp(s - most[None])
                w_buf[here, :] = w.reshape(SB, 2 * TQ)
                sums[at, :] = jnp.sum(w, 0)
                deltas[at, :] = jnp.sum(w * dp_buf[here, :].reshape(SB // 8, 8, 2 * TQ), 0)
                tops[at, :] = most
                top = jnp.maximum(top, most)
            return top

        def score_step(j, top):
            scores(j)
            return weights(j, top)

        top = lax.fori_loop(0, steps, score_step, jnp.full((8, 2 * TQ), -3e38, jnp.float32))
        top = jnp.max(top, 0, keepdims=True)

        def total_step(j, carry):
            total, delta = carry
            for b in range(TK // SB):
                at = pl.ds(pl.multiple_of((j * (TK // SB) + b) * 8, 8), 8)
                factor = jnp.exp(tops[at, :] - top)
                tops[at, :] = factor
                total = total + factor * sums[at, :]
                delta = delta + factor * deltas[at, :]
            return total, delta

        none = jnp.zeros((8, 2 * TQ), jnp.float32)
        total, delta = lax.fori_loop(0, steps, total_step, (none, none))
        inverse = 1.0 / jnp.sum(total, 0, keepdims=True)
        delta = jnp.sum(delta, 0, keepdims=True) * inverse
        att_acc[...] = jnp.zeros_like(att_acc)
        dq_acc[...] = jnp.zeros_like(dq_acc)

        def probs(j):
            for b in range(TK // SB):
                here = pl.ds(pl.multiple_of(j * TK + b * SB, SB), SB)
                at = pl.ds(pl.multiple_of((j * (TK // SB) + b) * 8, 8), 8)
                factor = tops[at, :] * inverse
                p = w_buf[here, :].reshape(SB // 8, 8, 2 * TQ) * factor[None]
                p = p.reshape(SB, 2 * TQ)
                p_buf[here, :] = p.astype(jnp.bfloat16)
                ds_buf[here, :] = (p * (dp_buf[here, :] - delta)).astype(jnp.bfloat16)

        def grads(j):
            keys = at_keys(j)
            p = p_buf[held(j), :]
            ds = ds_buf[held(j), :]
            for half in (0, 1):
                dims = slice(half * HEAD_DIM, (half + 1) * HEAD_DIM)
                cols = slice(half * TQ, (half + 1) * TQ)
                att_acc[dims, :] += dot_nn(vt[dims, keys], p[:, cols])
                dq_acc[dims, :] += dot_nn(kt[dims, keys], ds[:, cols])
            dk[keys, :] += dot_nn(ds, qd[...])
            dv[keys, :] += dot_nn(p, gs[...])

        def grad_step(j, c):
            probs(j)
            grads(j)
            return c

        lax.fori_loop(0, steps, grad_step, 0)
        att_ref[rows_here, :] = att_acc[...].T.astype(jnp.bfloat16)
        dq_ref[rows_here, :] = (dq_acc[...].T * scale).astype(jnp.bfloat16)
        return carry

    lax.fori_loop(0, tiles, one_tile, 0)
    for acc, mine, before, after in ((dk, dk_own, dk_before, dk_after),
                                     (dv, dv_own, dv_before, dv_after)):
        mine[...] = acc[halo : halo + own, :]
        before[...] = acc[:halo, :].astype(jnp.bfloat16)
        after[...] = acc[halo + own :, :].astype(jnp.bfloat16)


def attend(team, rows, args):
    halo = REACH * rows
    own = team * rows
    span = own + 2 * halo
    held = -(-min(2 * halo + TQ + LANES + TK, span + TK) // TK) * TK
    f = jnp.float32
    scratch = [
        pltpu.VMEM((held, 2 * TQ), f),
        pltpu.VMEM((held, 2 * TQ), f),
        pltpu.VMEM((held, 2 * TQ), f),
        pltpu.VMEM((held, 2 * TQ), jnp.bfloat16),
        pltpu.VMEM((held, 2 * TQ), jnp.bfloat16),
        pltpu.VMEM((held // SB * 8, 2 * TQ), f),
        pltpu.VMEM((held // SB * 8, 2 * TQ), f),
        pltpu.VMEM((held // SB * 8, 2 * TQ), f),
        pltpu.VMEM((span, LANES), f),
        pltpu.VMEM((span, LANES), f),
        pltpu.VMEM((LANES, TQ), f),
        pltpu.VMEM((LANES, TQ), f),
        pltpu.VMEM((2 * LANES, 2 * TQ), jnp.bfloat16),
        pltpu.VMEM((2 * TQ, LANES), jnp.bfloat16),
        pltpu.VMEM((2 * TQ, LANES), jnp.bfloat16),
        pltpu.SMEM((own // TQ,), jnp.int32),
        pltpu.SMEM((own // TQ,), jnp.int32),
    ]
    outs = (bf16(own, LANES), bf16(own, LANES), f32(own, LANES), f32(own, LANES)) + (
        bf16(halo, LANES),) * 4
    return pl.pallas_call(
        lambda *refs: attend_kernel(team, rows, *refs),
        name="attend",
        out_shape=outs,
        in_specs=[VMEM] * len(args),
        out_specs=(VMEM,) * len(outs),
        scratch_shapes=scratch,
        compiler_params=pltpu.CompilerParams(vmem_limit_bytes=40 * 1024 * 1024),
        cost_estimate=pl.CostEstimate(
            flops=60_000_000_000, bytes_accessed=12_000_000, transcendentals=8_000_000),
    )(*args)


def scatter_kernel(count, team, *refs):
    att, dq, dk_own, dv_own, dk_before, dk_after, dv_before, dv_after = refs[:8]
    outs, (above_in, below_in, staged, send, recv, halo_send, halo_recv, local) = refs[8:12], refs[12:]
    me, base, pos, up, down = place(count, team)
    above = me + team < count
    below = me >= team
    rows = outs[0].shape[0]
    halo = REACH * rows
    own = team * rows
    greet(base, pos, team, up, down)

    def halo_copies(t):
        before, after = ((dk_before, dk_after), (dv_before, dv_after))[t]
        return (remote(before, above_in.at[t], halo_send.at[t, 0], halo_recv.at[t, 0], down),
                remote(after, below_in.at[t], halo_send.at[t, 1], halo_recv.at[t, 1], up))

    for t in range(2):
        down_copy, up_copy = halo_copies(t)
        pl.when(below)(down_copy.start)
        pl.when(above)(up_copy.start)
    copies = []

    def spread(t, src):
        for step in range(1, team):
            mate = lax.rem(pos + step, team)
            part = src.at[pl.ds(pl.multiple_of(mate * rows, 16), rows), :]
            copy = remote(part, outs[t].at[:, lanes_of(pos)], send.at[t, step], recv.at[t, step],
                          base + mate)
            copy.start()
            copies.append(copy)
        part = src.at[pl.ds(pl.multiple_of(pos * rows, 16), rows), :]
        copy = pltpu.make_async_copy(part, outs[t].at[:, lanes_of(pos)], local.at[t])
        copy.start()
        return copy

    mine = [spread(0, att), spread(1, dq)]
    for t, src in enumerate((dk_own, dv_own)):
        down_copy, up_copy = halo_copies(t)
        dst = staged.at[t]
        dst[halo : own - halo, :] = src[halo : own - halo, :].astype(jnp.bfloat16)

        @pl.when(above)
        def _():
            down_copy.wait_recv()
            dst[own - halo :, :] = (src[own - halo :, :] + above_in[t].astype(jnp.float32)
                                    ).astype(jnp.bfloat16)

        @pl.when(jnp.logical_not(above))
        def _():
            dst[own - halo :, :] = src[own - halo :, :].astype(jnp.bfloat16)

        @pl.when(below)
        def _():
            up_copy.wait_recv()
            dst[:halo, :] = (src[:halo, :] + below_in[t].astype(jnp.float32)).astype(jnp.bfloat16)

        @pl.when(jnp.logical_not(below))
        def _():
            dst[:halo, :] = src[:halo, :].astype(jnp.bfloat16)

        mine.append(spread(2 + t, dst))
    for copy in mine:
        copy.wait()
    for copy in copies:
        copy.wait_recv()
        copy.wait_send()
    for t in range(2):
        down_copy, up_copy = halo_copies(t)
        pl.when(below)(down_copy.wait_send)
        pl.when(above)(up_copy.wait_send)


def scatter(count, team, rows, arrays):
    halo = REACH * rows
    return pl.pallas_call(
        lambda *refs: scatter_kernel(count, team, *refs),
        out_shape=(bf16(rows, team * LANES),) * 4,
        in_specs=[VMEM] * 8,
        out_specs=(VMEM,) * 4,
        scratch_shapes=[
            pltpu.VMEM((2, halo, LANES), jnp.bfloat16),
            pltpu.VMEM((2, halo, LANES), jnp.bfloat16),
            pltpu.VMEM((2, team * rows, LANES), jnp.bfloat16),
            pltpu.SemaphoreType.DMA((4, team)),
            pltpu.SemaphoreType.DMA((4, team)),
            pltpu.SemaphoreType.DMA((2, 2)),
            pltpu.SemaphoreType.DMA((2, 2)),
            pltpu.SemaphoreType.DMA((4,)),
        ],
        compiler_params=pltpu.CompilerParams(
            collective_id=1, has_side_effects=True, vmem_limit_bytes=20 * 1024 * 1024),
        name="scatter",
    )(*arrays)


def settle(arrays):
    def kernel(*refs):
        ins, outs, sems = refs[:4], refs[4:8], refs[8]
        copies = [pltpu.make_async_copy(a, b, sems.at[i]) for i, (a, b) in enumerate(zip(ins, outs))]
        for copy in copies:
            copy.start()
        for copy in copies:
            copy.wait()

    return pl.pallas_call(
        kernel,
        name="settle",
        out_shape=tuple(jax.ShapeDtypeStruct(a.shape, a.dtype) for a in arrays),
        in_specs=[VMEM] * 4,
        out_specs=(HBM,) * 4,
        scratch_shapes=[pltpu.SemaphoreType.DMA((4,))],
        compiler_params=pltpu.CompilerParams(vmem_limit_bytes=4 * 1024 * 1024),
    )(*arrays)


def shards(queries, keys, values, out_grad, image_ids):
    rows, features = queries.shape
    count = lax.axis_size("img")
    team = features // LANES
    tags = jnp.pad((image_ids + 1).reshape(rows // LANES, LANES),
                   ((0, TAG_ROWS - rows // LANES), (0, 0)), constant_values=NO_TAG)
    gathered = gather(count, team, tags, (keys, values, queries, out_grad))
    results = attend(team, rows, gathered)
    attended, query_grad, key_grad, value_grad = scatter(count, team, rows, results)
    return settle((attended, query_grad, key_grad, value_grad))


def solution(mesh):
    in_specs = (P("img", None), P("img", None), P("img", None), P("img", None), P("img"))
    out_specs = (P("img", None), P("img", None), P("img", None), P("img", None))
    return jax.shard_map(shards, mesh=mesh, in_specs=in_specs, out_specs=out_specs, check_vma=False)
```

```python
import math

import jax
import jax.numpy as jnp
from jax import lax
from jax.experimental import pallas as pl
from jax.experimental.pallas import tpu as pltpu
from jax.sharding import PartitionSpec as P

HEAD_DIM = 64
REACH = 3
LANES = 128
TAG_ROWS = 8
TQ = 256
TK = 256
SB = 128
WHOLE = 6
NO_TAG = 1 << 30
OUTSIDE = -1e30
MESH = pl.DeviceIdType.MESH
VMEM = pl.BlockSpec(memory_space=pltpu.VMEM)
ANY = pl.BlockSpec(memory_space=pl.ANY)
HBM = pl.BlockSpec(memory_space=pltpu.HBM)


def dot_nt(a, b):
    return lax.dot_general(a, b, (((1,), (1,)), ((), ())), preferred_element_type=jnp.float32)


def dot_nn(a, b):
    return lax.dot_general(a, b, (((1,), (0,)), ((), ())), preferred_element_type=jnp.float32)


def bf16(*shape):
    return jax.ShapeDtypeStruct(shape, jnp.bfloat16)


def f32(*shape):
    return jax.ShapeDtypeStruct(shape, jnp.float32)


def greet(base, pos, team, up, down):
    barrier = pltpu.get_barrier_semaphore()
    for step in range(1, team):
        mate = base + lax.rem(pos + step, team)
        pl.semaphore_signal(barrier, inc=1, device_id=(mate,), device_id_type=MESH)
    pl.semaphore_signal(barrier, inc=1, device_id=(up,), device_id_type=MESH)
    pl.semaphore_signal(barrier, inc=1, device_id=(down,), device_id_type=MESH)
    pl.semaphore_wait(barrier, team + 1)


def place(count, team):
    me = lax.axis_index("img")
    pos = lax.rem(me, team)
    return me, me - pos, pos, lax.rem(me + team, count), lax.rem(me + count - team, count)


def remote(src, dst, send_sem, recv_sem, device):
    return pltpu.make_async_remote_copy(
        src_ref=src, dst_ref=dst, send_sem=send_sem, recv_sem=recv_sem,
        device_id=(device,), device_id_type=MESH)


def lanes_of(pos):
    return pl.ds(pl.multiple_of(pos * LANES, LANES), LANES)


def gather_kernel(count, team, *refs):
    ins, outs = refs[:5], refs[5:10]
    kt, vt, qt, marks = refs[10:14]
    send, recv, halo_send, halo_recv, local = refs[14:]
    tags, kw, vw, _, _ = outs
    me, base, pos, up, down = place(count, team)
    above = me + team < count
    below = me >= team
    greet(base, pos, team, up, down)
    rows = [src.shape[0] for src in ins]
    halos = [REACH * r if t < 3 else 0 for t, r in enumerate(rows)]
    copies, own = [], []
    for t, (src, dst) in enumerate(zip(ins, outs)):
        mine = pl.ds(pl.multiple_of(halos[t] + pos * rows[t], 8), rows[t])
        for step in range(1, team):
            mate = lax.rem(pos + step, team)
            part = src if t == 0 else src.at[:, lanes_of(mate)]
            copy = remote(part, dst.at[mine, :], send.at[t, step], recv.at[t, step], base + mate)
            copy.start()
            copies.append(copy)
        part = src if t == 0 else src.at[:, lanes_of(pos)]
        copy = pltpu.make_async_copy(part, dst.at[mine, :], local.at[t])
        copy.start()
        own.append(copy)

    def halo_copies(t):
        dst, r, h = outs[t], rows[t], halos[t]
        down_copy = remote(dst.at[pl.ds(h, h), :], dst.at[pl.ds(h + team * r, h), :],
                           halo_send.at[t, 0], halo_recv.at[t, 0], down)
        up_copy = remote(dst.at[pl.ds(team * r, h), :], dst.at[pl.ds(0, h), :],
                         halo_send.at[t, 1], halo_recv.at[t, 1], up)
        return down_copy, up_copy

    def arrived(t):
        for copy in copies[t * (team - 1) : (t + 1) * (team - 1)]:
            copy.wait_recv()
        own[t].wait()

    def forward(t):
        down_copy, up_copy = halo_copies(t)
        pl.when(below)(down_copy.start)
        pl.when(above)(up_copy.start)

    def halo_arrived(t):
        down_copy, up_copy = halo_copies(t)
        pl.when(above)(down_copy.wait_recv)
        pl.when(below)(up_copy.wait_recv)

    def flip(src, dst, start, size):
        def step(i, c):
            for u in range(3):
                at = pl.ds(pl.multiple_of(start + (3 * i + u) * LANES, LANES), LANES)
                dst[:, at] = src[at, :].astype(jnp.float32).T.astype(jnp.bfloat16)
            return c
        lax.fori_loop(0, size // LANES // 3, step, 0)

    span = kw.shape[0]
    halo = halos[1]
    inner = span - 2 * halo

    @pl.when(jnp.logical_not(below))
    def _():
        kw[:halo, :] = jnp.zeros((halo, LANES), jnp.bfloat16)
        vw[:halo, :] = jnp.zeros((halo, LANES), jnp.bfloat16)
        used = lax.rem(lax.broadcasted_iota(jnp.int32, (halos[0], LANES), 0), TAG_ROWS)
        tags[: halos[0], :] = jnp.where(used < rows[1] // LANES, 0, NO_TAG)

    @pl.when(jnp.logical_not(above))
    def _():
        kw[halo + inner :, :] = jnp.zeros((halo, LANES), jnp.bfloat16)
        vw[halo + inner :, :] = jnp.zeros((halo, LANES), jnp.bfloat16)
        tags[halos[0] + team * rows[0] :, :] = jnp.full((halos[0], LANES), NO_TAG, jnp.int32)

    arrived(0)
    forward(0)
    arrived(1)
    forward(1)
    halo_arrived(0)
    ids = lax.broadcasted_iota(jnp.int32, (LANES, LANES), 0)

    def mark(i, c):
        for u in range(rows[1] // LANES):
            at = pl.ds(pl.multiple_of(i * rows[1] + u * LANES, LANES), LANES)
            tag = tags[pl.ds(i * TAG_ROWS + u, 1), :]
            outside = (tag <= 0) | (tag >= NO_TAG)
            hit = jnp.where((ids == lax.rem(tag, LANES)) | outside, 1.0, 0.0)
            marks[at, :] = hit.T.astype(jnp.bfloat16)
        return c

    lax.fori_loop(0, span // rows[1], mark, 0)
    flip(kw, kt, halo, inner)
    arrived(2)
    forward(2)
    halo_arrived(1)
    flip(kw, kt, 0, halo)
    flip(kw, kt, halo + inner, halo)
    flip(vw, vt, halo, inner)
    arrived(3)
    flip(outs[3], qt, 0, inner)
    halo_arrived(2)
    flip(vw, vt, 0, halo)
    flip(vw, vt, halo + inner, halo)
    arrived(4)
    for t in range(3):
        down_copy, up_copy = halo_copies(t)
        pl.when(below)(down_copy.wait_send)
        pl.when(above)(up_copy.wait_send)
    for copy in copies:
        copy.wait_send()


def gather(count, team, tags, arrays):
    rows = arrays[0].shape[0]
    span = (team + 2 * REACH) * rows
    return pl.pallas_call(
        lambda *refs: gather_kernel(count, team, *refs),
        out_shape=(
            jax.ShapeDtypeStruct(((team + 2 * REACH) * TAG_ROWS, LANES), jnp.int32),
            bf16(span, LANES), bf16(span, LANES), bf16(team * rows, LANES), bf16(team * rows, LANES),
            bf16(LANES, span), bf16(LANES, span), bf16(LANES, team * rows), bf16(span, LANES)),
        in_specs=[VMEM] + [HBM] * 4,
        out_specs=(VMEM,) * 9,
        scratch_shapes=[
            pltpu.SemaphoreType.DMA((5, team)),
            pltpu.SemaphoreType.DMA((5, team)),
            pltpu.SemaphoreType.DMA((3, 2)),
            pltpu.SemaphoreType.DMA((3, 2)),
            pltpu.SemaphoreType.DMA((5,)),
        ],
        compiler_params=pltpu.CompilerParams(
            collective_id=0, has_side_effects=True, vmem_limit_bytes=16 * 1024 * 1024),
        name="gather",
    )(tags, *arrays)


def attend_kernel(team, rows, *refs):
    tags, kw, vw, qw, gw, kt, vt, qt, marks = refs[:9]
    att_ref, dq_ref, dk_own, dv_own, dk_before, dk_after, dv_before, dv_after = refs[9:17]
    (s_buf, dp_buf, w_buf, p_buf, ds_buf, tops, sums, deltas, dk, dv, att_acc, dq_acc,
     qs, gs, qd, begins, ends) = refs[17:]
    halo = REACH * rows
    own = team * rows
    span = own + 2 * halo
    scale = 1.0 / math.sqrt(HEAD_DIM)
    low = lax.broadcasted_iota(jnp.int32, (TQ, LANES), 1) < HEAD_DIM
    ids = lax.broadcasted_iota(jnp.int32, (LANES, LANES), 0)
    tiles = own // TQ

    def tag_row(row):
        return (row // rows + REACH) * TAG_ROWS + row % rows // LANES

    for tile in range(tiles):
        first = tags[tag_row(tile * TQ) : tag_row(tile * TQ) + 1, :1]
        at = tag_row(tile * TQ + TQ - 1)
        final = tags[at : at + 1, LANES - 1 :]
        every = tags[...]
        begins[tile] = jnp.sum((every < first).astype(jnp.int32))
        ends[tile] = jnp.sum((every <= final).astype(jnp.int32))

    dk[...] = jnp.zeros_like(dk)
    dv[...] = jnp.zeros_like(dv)

    def one_tile(tile, carry):
        row0 = pl.multiple_of(tile * TQ, TQ)
        rows_here = pl.ds(row0, TQ)
        key0 = (begins[tile] // LANES) * LANES
        steps = (ends[tile] - key0 + TK - 1) // TK
        key0 = jnp.minimum(key0, span - steps * TK)

        q = qw[rows_here, :].astype(jnp.float32) * scale
        g = gw[rows_here, :].astype(jnp.float32)
        qd[:TQ, :] = jnp.where(low, q, 0.0).astype(jnp.bfloat16)
        qd[TQ:, :] = jnp.where(low, 0.0, q).astype(jnp.bfloat16)
        gs[:TQ, :] = jnp.where(low, g, 0.0).astype(jnp.bfloat16)
        gs[TQ:, :] = jnp.where(low, 0.0, g).astype(jnp.bfloat16)
        across = (qt[:, rows_here].astype(jnp.float32) * scale).astype(jnp.bfloat16)
        nothing = jnp.zeros((HEAD_DIM, TQ), jnp.bfloat16)
        qs[:HEAD_DIM, :TQ] = across[:HEAD_DIM]
        qs[HEAD_DIM:LANES, :TQ] = nothing
        qs[:HEAD_DIM, TQ:] = nothing
        qs[HEAD_DIM:LANES, TQ:] = across[HEAD_DIM:]
        for u in range(TQ // LANES):
            strip = tile * (TQ // LANES) + u
            per = rows // LANES
            tag = tags[pl.ds((strip // per + REACH) * TAG_ROWS + lax.rem(strip, per), 1), :]
            apart = jnp.where(ids == lax.rem(tag, LANES), 0.0, OUTSIDE).astype(jnp.bfloat16)
            qs[LANES:, u * LANES : (u + 1) * LANES] = apart
            qs[LANES:, TQ + u * LANES : TQ + (u + 1) * LANES] = apart

        def scores(j, many):
            keys = pl.ds(pl.multiple_of(key0 + j * TK, LANES), many * TK)
            here = pl.ds(pl.multiple_of(j * TK, TK), many * TK)
            s_buf[here, :] = dot_nn(jnp.concatenate([kw[keys, :], marks[keys, :]], 1), qs[...])
            dp_buf[here, :] = dot_nt(vw[keys, :], gs[...])

        def weights(j, top):
            here = pl.ds(pl.multiple_of(j * SB, SB), SB)
            at = pl.ds(pl.multiple_of(j * 8, 8), 8)
            s = s_buf[here, :].reshape(SB // 8, 8, 2 * TQ)
            most = jnp.max(s, 0)
            w = jnp.exp(s - most[None])
            w_buf[here, :] = w.reshape(SB, 2 * TQ)
            sums[at, :] = jnp.sum(w, 0)
            deltas[at, :] = jnp.sum(w * dp_buf[here, :].reshape(SB // 8, 8, 2 * TQ), 0)
            tops[at, :] = most
            return jnp.maximum(top, most)

        def sweep(body):
            def whole_step(j, c):
                body(WHOLE * j, WHOLE)
                return c

            lax.fori_loop(0, steps // WHOLE, whole_step, 0)
            for rest in range(1, WHOLE):
                @pl.when(lax.rem(steps, WHOLE) == rest)
                def _():
                    body(steps - rest, rest)

        sweep(scores)
        parts = steps * (TK // SB)
        top = lax.fori_loop(0, parts, weights, jnp.full((8, 2 * TQ), -3e38, jnp.float32))
        top = jnp.max(top, 0, keepdims=True)

        def total_step(j, carry):
            total, delta = carry
            for b in range(TK // SB):
                at = pl.ds(pl.multiple_of((j * (TK // SB) + b) * 8, 8), 8)
                factor = jnp.exp(tops[at, :] - top)
                tops[at, :] = factor
                total = total + factor * sums[at, :]
                delta = delta + factor * deltas[at, :]
            return total, delta

        none = jnp.zeros((8, 2 * TQ), jnp.float32)
        total, delta = lax.fori_loop(0, steps, total_step, (none, none))
        inverse = 1.0 / jnp.sum(total, 0, keepdims=True)
        delta = jnp.sum(delta, 0, keepdims=True) * inverse
        att_acc[...] = jnp.zeros_like(att_acc)
        dq_acc[...] = jnp.zeros_like(dq_acc)

        def probs(j, c):
            here = pl.ds(pl.multiple_of(j * SB, SB), SB)
            factor = tops[pl.ds(pl.multiple_of(j * 8, 8), 8), :] * inverse
            p = w_buf[here, :].reshape(SB // 8, 8, 2 * TQ) * factor[None]
            p = p.reshape(SB, 2 * TQ)
            p_buf[here, :] = p.astype(jnp.bfloat16)
            ds_buf[here, :] = (p * (dp_buf[here, :] - delta)).astype(jnp.bfloat16)
            return c

        def grads(j, many):
            keys = pl.ds(pl.multiple_of(key0 + j * TK, LANES), many * TK)
            here = pl.ds(pl.multiple_of(j * TK, TK), many * TK)
            p = p_buf[here, :]
            ds = ds_buf[here, :]
            dk[keys, :] += dot_nn(ds, qd[...])
            dv[keys, :] += dot_nn(p, gs[...])
            for half in (0, 1):
                dims = slice(half * HEAD_DIM, (half + 1) * HEAD_DIM)
                cols = slice(half * TQ, (half + 1) * TQ)
                att_acc[dims, :] += dot_nn(vt[dims, keys], p_buf[here, cols])
                dq_acc[dims, :] += dot_nn(kt[dims, keys], ds_buf[here, cols])

        lax.fori_loop(0, parts, probs, 0)
        sweep(grads)
        att_ref[rows_here, :] = att_acc[...].T.astype(jnp.bfloat16)
        dq_ref[rows_here, :] = (dq_acc[...].T * scale).astype(jnp.bfloat16)
        return carry

    lax.fori_loop(0, tiles, one_tile, 0)
    for acc, mine, before, after in ((dk, dk_own, dk_before, dk_after),
                                     (dv, dv_own, dv_before, dv_after)):
        mine[...] = acc[halo : halo + own, :]
        before[...] = acc[:halo, :].astype(jnp.bfloat16)
        after[...] = acc[halo + own :, :].astype(jnp.bfloat16)


def attend(team, rows, args):
    halo = REACH * rows
    own = team * rows
    span = own + 2 * halo
    held = -(-min(2 * halo + TQ + LANES + TK, span + TK) // TK) * TK
    f = jnp.float32
    scratch = [
        pltpu.VMEM((held, 2 * TQ), f),
        pltpu.VMEM((held, 2 * TQ), f),
        pltpu.VMEM((held, 2 * TQ), f),
        pltpu.VMEM((held, 2 * TQ), jnp.bfloat16),
        pltpu.VMEM((held, 2 * TQ), jnp.bfloat16),
        pltpu.VMEM((held // SB * 8, 2 * TQ), f),
        pltpu.VMEM((held // SB * 8, 2 * TQ), f),
        pltpu.VMEM((held // SB * 8, 2 * TQ), f),
        pltpu.VMEM((span, LANES), f),
        pltpu.VMEM((span, LANES), f),
        pltpu.VMEM((LANES, TQ), f),
        pltpu.VMEM((LANES, TQ), f),
        pltpu.VMEM((2 * LANES, 2 * TQ), jnp.bfloat16),
        pltpu.VMEM((2 * TQ, LANES), jnp.bfloat16),
        pltpu.VMEM((2 * TQ, LANES), jnp.bfloat16),
        pltpu.SMEM((own // TQ,), jnp.int32),
        pltpu.SMEM((own // TQ,), jnp.int32),
    ]
    outs = (bf16(own, LANES), bf16(own, LANES), f32(own, LANES), f32(own, LANES)) + (
        bf16(halo, LANES),) * 4
    return pl.pallas_call(
        lambda *refs: attend_kernel(team, rows, *refs),
        name="attend",
        out_shape=outs,
        in_specs=[VMEM] * len(args),
        out_specs=(VMEM,) * len(outs),
        scratch_shapes=scratch,
        compiler_params=pltpu.CompilerParams(vmem_limit_bytes=35 * 1024 * 1024),
        cost_estimate=pl.CostEstimate(
            flops=60_000_000_000, bytes_accessed=12_000_000, transcendentals=8_000_000),
    )(*args)


def scatter_kernel(count, team, *refs):
    att, dq, dk_own, dv_own, dk_before, dk_after, dv_before, dv_after = refs[:8]
    outs, (above_in, below_in, staged, send, recv, halo_send, halo_recv, local) = refs[8:12], refs[12:]
    me, base, pos, up, down = place(count, team)
    above = me + team < count
    below = me >= team
    rows = outs[0].shape[0]
    halo = REACH * rows
    own = team * rows
    greet(base, pos, team, up, down)

    def halo_copies(t):
        before, after = ((dk_before, dk_after), (dv_before, dv_after))[t]
        return (remote(before, above_in.at[t], halo_send.at[t, 0], halo_recv.at[t, 0], down),
                remote(after, below_in.at[t], halo_send.at[t, 1], halo_recv.at[t, 1], up))

    for t in range(2):
        down_copy, up_copy = halo_copies(t)
        pl.when(below)(down_copy.start)
        pl.when(above)(up_copy.start)
    copies = []

    def spread(t, src):
        for step in range(1, team):
            mate = lax.rem(pos + step, team)
            part = src.at[pl.ds(pl.multiple_of(mate * rows, 16), rows), :]
            copy = remote(part, outs[t].at[:, lanes_of(pos)], send.at[t, step], recv.at[t, step],
                          base + mate)
            copy.start()
            copies.append(copy)
        part = src.at[pl.ds(pl.multiple_of(pos * rows, 16), rows), :]
        copy = pltpu.make_async_copy(part, outs[t].at[:, lanes_of(pos)], local.at[t])
        copy.start()
        return copy

    mine = [spread(0, att), spread(1, dq)]
    for t, src in enumerate((dk_own, dv_own)):
        down_copy, up_copy = halo_copies(t)
        dst = staged.at[t]
        dst[halo : own - halo, :] = src[halo : own - halo, :].astype(jnp.bfloat16)

        @pl.when(above)
        def _():
            down_copy.wait_recv()
            dst[own - halo :, :] = (src[own - halo :, :] + above_in[t].astype(jnp.float32)
                                    ).astype(jnp.bfloat16)

        @pl.when(jnp.logical_not(above))
        def _():
            dst[own - halo :, :] = src[own - halo :, :].astype(jnp.bfloat16)

        @pl.when(below)
        def _():
            up_copy.wait_recv()
            dst[:halo, :] = (src[:halo, :] + below_in[t].astype(jnp.float32)).astype(jnp.bfloat16)

        @pl.when(jnp.logical_not(below))
        def _():
            dst[:halo, :] = src[:halo, :].astype(jnp.bfloat16)

        mine.append(spread(2 + t, dst))
    for copy in mine:
        copy.wait()
    for copy in copies:
        copy.wait_recv()
        copy.wait_send()
    for t in range(2):
        down_copy, up_copy = halo_copies(t)
        pl.when(below)(down_copy.wait_send)
        pl.when(above)(up_copy.wait_send)


def scatter(count, team, rows, arrays):
    halo = REACH * rows
    return pl.pallas_call(
        lambda *refs: scatter_kernel(count, team, *refs),
        out_shape=(bf16(rows, team * LANES),) * 4,
        in_specs=[VMEM] * 8,
        out_specs=(VMEM,) * 4,
        scratch_shapes=[
            pltpu.VMEM((2, halo, LANES), jnp.bfloat16),
            pltpu.VMEM((2, halo, LANES), jnp.bfloat16),
            pltpu.VMEM((2, team * rows, LANES), jnp.bfloat16),
            pltpu.SemaphoreType.DMA((4, team)),
            pltpu.SemaphoreType.DMA((4, team)),
            pltpu.SemaphoreType.DMA((2, 2)),
            pltpu.SemaphoreType.DMA((2, 2)),
            pltpu.SemaphoreType.DMA((4,)),
        ],
        compiler_params=pltpu.CompilerParams(
            collective_id=1, has_side_effects=True, vmem_limit_bytes=20 * 1024 * 1024),
        name="scatter",
    )(*arrays)


def settle(arrays):
    def kernel(*refs):
        ins, outs, sems = refs[:4], refs[4:8], refs[8]
        copies = [pltpu.make_async_copy(a, b, sems.at[i]) for i, (a, b) in enumerate(zip(ins, outs))]
        for copy in copies:
            copy.start()
        for copy in copies:
            copy.wait()

    return pl.pallas_call(
        kernel,
        name="settle",
        out_shape=tuple(jax.ShapeDtypeStruct(a.shape, a.dtype) for a in arrays),
        in_specs=[VMEM] * 4,
        out_specs=(HBM,) * 4,
        scratch_shapes=[pltpu.SemaphoreType.DMA((4,))],
        compiler_params=pltpu.CompilerParams(vmem_limit_bytes=4 * 1024 * 1024),
    )(*arrays)


def shards(queries, keys, values, out_grad, image_ids):
    rows, features = queries.shape
    count = lax.axis_size("img")
    team = features // LANES
    tags = jnp.pad((image_ids + 1).reshape(rows // LANES, LANES),
                   ((0, TAG_ROWS - rows // LANES), (0, 0)), constant_values=NO_TAG)
    gathered = gather(count, team, tags, (keys, values, queries, out_grad))
    results = attend(team, rows, gathered)
    attended, query_grad, key_grad, value_grad = scatter(count, team, rows, results)
    return settle((attended, query_grad, key_grad, value_grad))


def solution(mesh):
    in_specs = (P("img", None), P("img", None), P("img", None), P("img", None), P("img"))
    out_specs = (P("img", None), P("img", None), P("img", None), P("img", None))
    return jax.shard_map(shards, mesh=mesh, in_specs=in_specs, out_specs=out_specs, check_vma=False)
```

```python
import math

import jax
import jax.numpy as jnp
from jax import lax
from jax.experimental import pallas as pl
from jax.experimental.pallas import tpu as pltpu
from jax.sharding import PartitionSpec as P

HEAD_DIM = 64
REACH = 3
LANES = 128
TAG_ROWS = 8
TQ = 256
TK = 256
SB = 128
WHOLE = 6
NO_TAG = 1 << 30
OUTSIDE = -1e30
MESH = pl.DeviceIdType.MESH
VMEM = pl.BlockSpec(memory_space=pltpu.VMEM)
ANY = pl.BlockSpec(memory_space=pl.ANY)
HBM = pl.BlockSpec(memory_space=pltpu.HBM)


def dot_nt(a, b):
    return lax.dot_general(a, b, (((1,), (1,)), ((), ())), preferred_element_type=jnp.float32)


def dot_nn(a, b):
    return lax.dot_general(a, b, (((1,), (0,)), ((), ())), preferred_element_type=jnp.float32)


def bf16(*shape):
    return jax.ShapeDtypeStruct(shape, jnp.bfloat16)


def f32(*shape):
    return jax.ShapeDtypeStruct(shape, jnp.float32)


def greet(base, pos, team, up, down):
    barrier = pltpu.get_barrier_semaphore()
    for step in range(1, team):
        mate = base + lax.rem(pos + step, team)
        pl.semaphore_signal(barrier, inc=1, device_id=(mate,), device_id_type=MESH)
    pl.semaphore_signal(barrier, inc=1, device_id=(up,), device_id_type=MESH)
    pl.semaphore_signal(barrier, inc=1, device_id=(down,), device_id_type=MESH)
    pl.semaphore_wait(barrier, team + 1)


def place(count, team):
    me = lax.axis_index("img")
    pos = lax.rem(me, team)
    return me, me - pos, pos, lax.rem(me + team, count), lax.rem(me + count - team, count)


def remote(src, dst, send_sem, recv_sem, device):
    return pltpu.make_async_remote_copy(
        src_ref=src, dst_ref=dst, send_sem=send_sem, recv_sem=recv_sem,
        device_id=(device,), device_id_type=MESH)


def lanes_of(pos):
    return pl.ds(pl.multiple_of(pos * LANES, LANES), LANES)


def gather_kernel(count, team, *refs):
    ins, outs = refs[:5], refs[5:10]
    kt, vt, qt, marks = refs[10:14]
    send, recv, halo_send, halo_recv, local = refs[14:]
    tags, kw, vw, _, _ = outs
    me, base, pos, up, down = place(count, team)
    above = me + team < count
    below = me >= team
    greet(base, pos, team, up, down)
    rows = [src.shape[0] for src in ins]
    halos = [REACH * r if t < 3 else 0 for t, r in enumerate(rows)]
    copies, own = [], []
    for t, (src, dst) in enumerate(zip(ins, outs)):
        mine = pl.ds(pl.multiple_of(halos[t] + pos * rows[t], 8), rows[t])
        for step in range(1, team):
            mate = lax.rem(pos + step, team)
            part = src if t == 0 else src.at[:, lanes_of(mate)]
            copy = remote(part, dst.at[mine, :], send.at[t, step], recv.at[t, step], base + mate)
            copy.start()
            copies.append(copy)
        part = src if t == 0 else src.at[:, lanes_of(pos)]
        copy = pltpu.make_async_copy(part, dst.at[mine, :], local.at[t])
        copy.start()
        own.append(copy)

    def halo_copies(t):
        dst, r, h = outs[t], rows[t], halos[t]
        down_copy = remote(dst.at[pl.ds(h, h), :], dst.at[pl.ds(h + team * r, h), :],
                           halo_send.at[t, 0], halo_recv.at[t, 0], down)
        up_copy = remote(dst.at[pl.ds(team * r, h), :], dst.at[pl.ds(0, h), :],
                         halo_send.at[t, 1], halo_recv.at[t, 1], up)
        return down_copy, up_copy

    def arrived(t):
        for copy in copies[t * (team - 1) : (t + 1) * (team - 1)]:
            copy.wait_recv()
        own[t].wait()

    def forward(t):
        down_copy, up_copy = halo_copies(t)
        pl.when(below)(down_copy.start)
        pl.when(above)(up_copy.start)

    def halo_arrived(t):
        down_copy, up_copy = halo_copies(t)
        pl.when(above)(down_copy.wait_recv)
        pl.when(below)(up_copy.wait_recv)

    def flip(src, dst, start, size):
        def step(i, c):
            for u in range(3):
                at = pl.ds(pl.multiple_of(start + (3 * i + u) * LANES, LANES), LANES)
                dst[:, at] = src[at, :].astype(jnp.float32).T.astype(jnp.bfloat16)
            return c
        lax.fori_loop(0, size // LANES // 3, step, 0)

    span = kw.shape[0]
    halo = halos[1]
    inner = span - 2 * halo

    @pl.when(jnp.logical_not(below))
    def _():
        kw[:halo, :] = jnp.zeros((halo, LANES), jnp.bfloat16)
        vw[:halo, :] = jnp.zeros((halo, LANES), jnp.bfloat16)
        used = lax.rem(lax.broadcasted_iota(jnp.int32, (halos[0], LANES), 0), TAG_ROWS)
        tags[: halos[0], :] = jnp.where(used < rows[1] // LANES, 0, NO_TAG)

    @pl.when(jnp.logical_not(above))
    def _():
        kw[halo + inner :, :] = jnp.zeros((halo, LANES), jnp.bfloat16)
        vw[halo + inner :, :] = jnp.zeros((halo, LANES), jnp.bfloat16)
        tags[halos[0] + team * rows[0] :, :] = jnp.full((halos[0], LANES), NO_TAG, jnp.int32)

    arrived(0)
    forward(0)
    arrived(1)
    forward(1)
    halo_arrived(0)
    ids = lax.broadcasted_iota(jnp.int32, (LANES, LANES), 0)

    def mark(i, c):
        for u in range(rows[1] // LANES):
            at = pl.ds(pl.multiple_of(i * rows[1] + u * LANES, LANES), LANES)
            tag = tags[pl.ds(i * TAG_ROWS + u, 1), :]
            outside = (tag <= 0) | (tag >= NO_TAG)
            hit = jnp.where((ids == lax.rem(tag, LANES)) | outside, 1.0, 0.0)
            marks[at, :] = hit.T.astype(jnp.bfloat16)
        return c

    lax.fori_loop(0, span // rows[1], mark, 0)
    flip(kw, kt, halo, inner)
    arrived(2)
    forward(2)
    halo_arrived(1)
    flip(kw, kt, 0, halo)
    flip(kw, kt, halo + inner, halo)
    flip(vw, vt, halo, inner)
    arrived(3)
    flip(outs[3], qt, 0, inner)
    halo_arrived(2)
    flip(vw, vt, 0, halo)
    flip(vw, vt, halo + inner, halo)
    arrived(4)
    for t in range(3):
        down_copy, up_copy = halo_copies(t)
        pl.when(below)(down_copy.wait_send)
        pl.when(above)(up_copy.wait_send)
    for copy in copies:
        copy.wait_send()


def gather(count, team, tags, arrays):
    rows = arrays[0].shape[0]
    span = (team + 2 * REACH) * rows
    return pl.pallas_call(
        lambda *refs: gather_kernel(count, team, *refs),
        out_shape=(
            jax.ShapeDtypeStruct(((team + 2 * REACH) * TAG_ROWS, LANES), jnp.int32),
            bf16(span, LANES), bf16(span, LANES), bf16(team * rows, LANES), bf16(team * rows, LANES),
            bf16(LANES, span), bf16(LANES, span), bf16(LANES, team * rows), bf16(span, LANES)),
        in_specs=[VMEM] * 5,
        out_specs=(VMEM,) * 9,
        scratch_shapes=[
            pltpu.SemaphoreType.DMA((5, team)),
            pltpu.SemaphoreType.DMA((5, team)),
            pltpu.SemaphoreType.DMA((3, 2)),
            pltpu.SemaphoreType.DMA((3, 2)),
            pltpu.SemaphoreType.DMA((5,)),
        ],
        compiler_params=pltpu.CompilerParams(
            collective_id=0, has_side_effects=True, vmem_limit_bytes=16 * 1024 * 1024),
        name="gather",
    )(tags, *arrays)


def attend_kernel(team, rows, *refs):
    tags, kw, vw, qw, gw, kt, vt, qt, marks = refs[:9]
    att_ref, dq_ref, dk_own, dv_own, dk_before, dk_after, dv_before, dv_after = refs[9:17]
    (s_buf, dp_buf, w_buf, p_buf, ds_buf, tops, sums, deltas, dk, dv, att_acc, dq_acc,
     qs, gs, qd, begins, ends) = refs[17:]
    halo = REACH * rows
    own = team * rows
    span = own + 2 * halo
    scale = 1.0 / math.sqrt(HEAD_DIM)
    low = lax.broadcasted_iota(jnp.int32, (TQ, LANES), 1) < HEAD_DIM
    ids = lax.broadcasted_iota(jnp.int32, (LANES, LANES), 0)
    tiles = own // TQ

    def tag_row(row):
        return (row // rows + REACH) * TAG_ROWS + row % rows // LANES

    for tile in range(tiles):
        first = tags[tag_row(tile * TQ) : tag_row(tile * TQ) + 1, :1]
        at = tag_row(tile * TQ + TQ - 1)
        final = tags[at : at + 1, LANES - 1 :]
        every = tags[...]
        begins[tile] = jnp.sum((every < first).astype(jnp.int32))
        ends[tile] = jnp.sum((every <= final).astype(jnp.int32))

    dk[...] = jnp.zeros_like(dk)
    dv[...] = jnp.zeros_like(dv)

    def one_tile(tile, carry):
        row0 = pl.multiple_of(tile * TQ, TQ)
        rows_here = pl.ds(row0, TQ)
        key0 = (begins[tile] // LANES) * LANES
        steps = (ends[tile] - key0 + TK - 1) // TK
        key0 = jnp.minimum(key0, span - steps * TK)

        q = qw[rows_here, :].astype(jnp.float32) * scale
        g = gw[rows_here, :].astype(jnp.float32)
        qd[:TQ, :] = jnp.where(low, q, 0.0).astype(jnp.bfloat16)
        qd[TQ:, :] = jnp.where(low, 0.0, q).astype(jnp.bfloat16)
        gs[:TQ, :] = jnp.where(low, g, 0.0).astype(jnp.bfloat16)
        gs[TQ:, :] = jnp.where(low, 0.0, g).astype(jnp.bfloat16)
        across = (qt[:, rows_here].astype(jnp.float32) * scale).astype(jnp.bfloat16)
        nothing = jnp.zeros((HEAD_DIM, TQ), jnp.bfloat16)
        qs[:HEAD_DIM, :TQ] = across[:HEAD_DIM]
        qs[HEAD_DIM:LANES, :TQ] = nothing
        qs[:HEAD_DIM, TQ:] = nothing
        qs[HEAD_DIM:LANES, TQ:] = across[HEAD_DIM:]
        for u in range(TQ // LANES):
            strip = tile * (TQ // LANES) + u
            per = rows // LANES
            tag = tags[pl.ds((strip // per + REACH) * TAG_ROWS + lax.rem(strip, per), 1), :]
            apart = jnp.where(ids == lax.rem(tag, LANES), 0.0, OUTSIDE).astype(jnp.bfloat16)
            qs[LANES:, u * LANES : (u + 1) * LANES] = apart
            qs[LANES:, TQ + u * LANES : TQ + (u + 1) * LANES] = apart

        def scores(j, many):
            keys = pl.ds(pl.multiple_of(key0 + j * TK, LANES), many * TK)
            here = pl.ds(pl.multiple_of(j * TK, TK), many * TK)
            s_buf[here, :] = dot_nn(jnp.concatenate([kw[keys, :], marks[keys, :]], 1), qs[...])
            dp_buf[here, :] = dot_nt(vw[keys, :], gs[...])

        def weights(j, many):
            for u in range(many * TK // SB):
                here = pl.ds(pl.multiple_of(j * TK + u * SB, SB), SB)
                at = pl.ds(pl.multiple_of(j * (TK // SB * 8) + u * 8, 8), 8)
                s = s_buf[here, :].reshape(SB // 8, 8, 2 * TQ)
                most = jnp.max(s, 0)
                w = jnp.exp(s - most[None])
                w_buf[here, :] = w.reshape(SB, 2 * TQ)
                sums[at, :] = jnp.sum(w, 0)
                deltas[at, :] = jnp.sum(w * dp_buf[here, :].reshape(SB // 8, 8, 2 * TQ), 0)
                tops[at, :] = most

        def score(j, many):
            for u in range(many):
                scores(j + u, 1)
                weights(j + u, 1)

        def sweep(body):
            def whole_step(j, c):
                body(WHOLE * j, WHOLE)
                return c

            lax.fori_loop(0, steps // WHOLE, whole_step, 0)
            for rest in range(1, WHOLE):
                @pl.when(lax.rem(steps, WHOLE) == rest)
                def _():
                    body(steps - rest, rest)

        sweep(score)
        parts = steps * (TK // SB)

        def top_step(j, top):
            return jnp.maximum(top, tops[pl.ds(pl.multiple_of(j * 8, 8), 8), :])

        top = lax.fori_loop(0, parts, top_step, jnp.full((8, 2 * TQ), -3e38, jnp.float32))
        top = jnp.max(top, 0, keepdims=True)

        def total_step(j, carry):
            total, delta = carry
            for b in range(TK // SB):
                at = pl.ds(pl.multiple_of((j * (TK // SB) + b) * 8, 8), 8)
                factor = jnp.exp(tops[at, :] - top)
                tops[at, :] = factor
                total = total + factor * sums[at, :]
                delta = delta + factor * deltas[at, :]
            return total, delta

        none = jnp.zeros((8, 2 * TQ), jnp.float32)
        total, delta = lax.fori_loop(0, steps, total_step, (none, none))
        inverse = 1.0 / jnp.sum(total, 0, keepdims=True)
        delta = jnp.sum(delta, 0, keepdims=True) * inverse
        att_acc[...] = jnp.zeros_like(att_acc)
        dq_acc[...] = jnp.zeros_like(dq_acc)

        def probs(j, c):
            here = pl.ds(pl.multiple_of(j * SB, SB), SB)
            factor = tops[pl.ds(pl.multiple_of(j * 8, 8), 8), :] * inverse
            p = w_buf[here, :].reshape(SB // 8, 8, 2 * TQ) * factor[None]
            p = p.reshape(SB, 2 * TQ)
            p_buf[here, :] = p.astype(jnp.bfloat16)
            ds_buf[here, :] = (p * (dp_buf[here, :] - delta)).astype(jnp.bfloat16)
            return c

        def grads(j, many):
            keys = pl.ds(pl.multiple_of(key0 + j * TK, LANES), many * TK)
            here = pl.ds(pl.multiple_of(j * TK, TK), many * TK)
            p = p_buf[here, :]
            ds = ds_buf[here, :]
            dk[keys, :] += dot_nn(ds, qd[...])
            dv[keys, :] += dot_nn(p, gs[...])
            for half in (0, 1):
                dims = slice(half * HEAD_DIM, (half + 1) * HEAD_DIM)
                cols = slice(half * TQ, (half + 1) * TQ)
                att_acc[dims, :] += dot_nn(vt[dims, keys], p_buf[here, cols])
                dq_acc[dims, :] += dot_nn(kt[dims, keys], ds_buf[here, cols])

        lax.fori_loop(0, parts, probs, 0)
        sweep(grads)
        att_ref[rows_here, :] = att_acc[...].T.astype(jnp.bfloat16)
        dq_ref[rows_here, :] = (dq_acc[...].T * scale).astype(jnp.bfloat16)
        return carry

    lax.fori_loop(0, tiles, one_tile, 0)
    for acc, mine, before, after in ((dk, dk_own, dk_before, dk_after),
                                     (dv, dv_own, dv_before, dv_after)):
        mine[...] = acc[halo : halo + own, :]
        before[...] = acc[:halo, :].astype(jnp.bfloat16)
        after[...] = acc[halo + own :, :].astype(jnp.bfloat16)


def attend(team, rows, args):
    halo = REACH * rows
    own = team * rows
    span = own + 2 * halo
    held = -(-min(2 * halo + TQ + LANES + TK, span + TK) // TK) * TK
    f = jnp.float32
    scratch = [
        pltpu.VMEM((held, 2 * TQ), f),
        pltpu.VMEM((held, 2 * TQ), f),
        pltpu.VMEM((held, 2 * TQ), f),
        pltpu.VMEM((held, 2 * TQ), jnp.bfloat16),
        pltpu.VMEM((held, 2 * TQ), jnp.bfloat16),
        pltpu.VMEM((held // SB * 8, 2 * TQ), f),
        pltpu.VMEM((held // SB * 8, 2 * TQ), f),
        pltpu.VMEM((held // SB * 8, 2 * TQ), f),
        pltpu.VMEM((span, LANES), f),
        pltpu.VMEM((span, LANES), f),
        pltpu.VMEM((LANES, TQ), f),
        pltpu.VMEM((LANES, TQ), f),
        pltpu.VMEM((2 * LANES, 2 * TQ), jnp.bfloat16),
        pltpu.VMEM((2 * TQ, LANES), jnp.bfloat16),
        pltpu.VMEM((2 * TQ, LANES), jnp.bfloat16),
        pltpu.SMEM((own // TQ,), jnp.int32),
        pltpu.SMEM((own // TQ,), jnp.int32),
    ]
    outs = (bf16(own, LANES), bf16(own, LANES), f32(own, LANES), f32(own, LANES)) + (
        bf16(halo, LANES),) * 4
    return pl.pallas_call(
        lambda *refs: attend_kernel(team, rows, *refs),
        name="attend",
        out_shape=outs,
        in_specs=[VMEM] * len(args),
        out_specs=(VMEM,) * len(outs),
        scratch_shapes=scratch,
        compiler_params=pltpu.CompilerParams(vmem_limit_bytes=35 * 1024 * 1024),
        cost_estimate=pl.CostEstimate(
            flops=60_000_000_000, bytes_accessed=12_000_000, transcendentals=8_000_000),
    )(*args)


def scatter_kernel(count, team, *refs):
    att, dq, dk_own, dv_own, dk_before, dk_after, dv_before, dv_after = refs[:8]
    outs, (above_in, below_in, staged, send, recv, halo_send, halo_recv, local) = refs[8:12], refs[12:]
    me, base, pos, up, down = place(count, team)
    above = me + team < count
    below = me >= team
    rows = outs[0].shape[0]
    halo = REACH * rows
    own = team * rows
    greet(base, pos, team, up, down)

    def halo_copies(t):
        before, after = ((dk_before, dk_after), (dv_before, dv_after))[t]
        return (remote(before, above_in.at[t], halo_send.at[t, 0], halo_recv.at[t, 0], down),
                remote(after, below_in.at[t], halo_send.at[t, 1], halo_recv.at[t, 1], up))

    for t in range(2):
        down_copy, up_copy = halo_copies(t)
        pl.when(below)(down_copy.start)
        pl.when(above)(up_copy.start)
    copies = []

    def spread(t, src):
        for step in range(1, team):
            mate = lax.rem(pos + step, team)
            part = src.at[pl.ds(pl.multiple_of(mate * rows, 16), rows), :]
            copy = remote(part, outs[t].at[:, lanes_of(pos)], send.at[t, step], recv.at[t, step],
                          base + mate)
            copy.start()
            copies.append(copy)
        part = src.at[pl.ds(pl.multiple_of(pos * rows, 16), rows), :]
        copy = pltpu.make_async_copy(part, outs[t].at[:, lanes_of(pos)], local.at[t])
        copy.start()
        return copy

    mine = [spread(0, att), spread(1, dq)]
    for t, src in enumerate((dk_own, dv_own)):
        down_copy, up_copy = halo_copies(t)
        dst = staged.at[t]
        dst[halo : own - halo, :] = src[halo : own - halo, :].astype(jnp.bfloat16)

        @pl.when(above)
        def _():
            down_copy.wait_recv()
            dst[own - halo :, :] = (src[own - halo :, :] + above_in[t].astype(jnp.float32)
                                    ).astype(jnp.bfloat16)

        @pl.when(jnp.logical_not(above))
        def _():
            dst[own - halo :, :] = src[own - halo :, :].astype(jnp.bfloat16)

        @pl.when(below)
        def _():
            up_copy.wait_recv()
            dst[:halo, :] = (src[:halo, :] + below_in[t].astype(jnp.float32)).astype(jnp.bfloat16)

        @pl.when(jnp.logical_not(below))
        def _():
            dst[:halo, :] = src[:halo, :].astype(jnp.bfloat16)

        mine.append(spread(2 + t, dst))
    for copy in mine:
        copy.wait()
    for copy in copies:
        copy.wait_recv()
        copy.wait_send()
    for t in range(2):
        down_copy, up_copy = halo_copies(t)
        pl.when(below)(down_copy.wait_send)
        pl.when(above)(up_copy.wait_send)


def scatter(count, team, rows, arrays):
    halo = REACH * rows
    return pl.pallas_call(
        lambda *refs: scatter_kernel(count, team, *refs),
        out_shape=(bf16(rows, team * LANES),) * 4,
        in_specs=[VMEM] * 8,
        out_specs=(VMEM,) * 4,
        scratch_shapes=[
            pltpu.VMEM((2, halo, LANES), jnp.bfloat16),
            pltpu.VMEM((2, halo, LANES), jnp.bfloat16),
            pltpu.VMEM((2, team * rows, LANES), jnp.bfloat16),
            pltpu.SemaphoreType.DMA((4, team)),
            pltpu.SemaphoreType.DMA((4, team)),
            pltpu.SemaphoreType.DMA((2, 2)),
            pltpu.SemaphoreType.DMA((2, 2)),
            pltpu.SemaphoreType.DMA((4,)),
        ],
        compiler_params=pltpu.CompilerParams(
            collective_id=1, has_side_effects=True, vmem_limit_bytes=20 * 1024 * 1024),
        name="scatter",
    )(*arrays)


def move(arrays, source, target, name, grant):
    def kernel(*refs):
        ins, outs, sems = refs[:4], refs[4:8], refs[8]
        copies = [pltpu.make_async_copy(a, b, sems.at[i]) for i, (a, b) in enumerate(zip(ins, outs))]
        for copy in copies:
            copy.start()
        for copy in copies:
            copy.wait()

    return pl.pallas_call(
        kernel,
        name=name,
        out_shape=tuple(jax.ShapeDtypeStruct(a.shape, a.dtype) for a in arrays),
        in_specs=[source] * 4,
        out_specs=(target,) * 4,
        scratch_shapes=[pltpu.SemaphoreType.DMA((4,))],
        compiler_params=pltpu.CompilerParams(vmem_limit_bytes=grant),
    )(*arrays)


def shards(queries, keys, values, out_grad, image_ids):
    rows, features = queries.shape
    count = lax.axis_size("img")
    team = features // LANES
    tags = jnp.pad((image_ids + 1).reshape(rows // LANES, LANES),
                   ((0, TAG_ROWS - rows // LANES), (0, 0)), constant_values=NO_TAG)
    arrays = move((keys, values, queries, out_grad), HBM, VMEM, "load", 53_200_000)
    gathered = gather(count, team, tags, arrays)
    results = attend(team, rows, gathered)
    attended, query_grad, key_grad, value_grad = scatter(count, team, rows, results)
    return move((attended, query_grad, key_grad, value_grad), VMEM, HBM, "settle", 4 * 1024 * 1024)


def solution(mesh):
    in_specs = (P("img", None), P("img", None), P("img", None), P("img", None), P("img"))
    out_specs = (P("img", None), P("img", None), P("img", None), P("img", None))
    return jax.shard_map(shards, mesh=mesh, in_specs=in_specs, out_specs=out_specs, check_vma=False)
```

```python
import math

import jax
import jax.numpy as jnp
from jax import lax
from jax.experimental import pallas as pl
from jax.experimental.pallas import tpu as pltpu
from jax.sharding import PartitionSpec as P

HEAD_DIM = 64
REACH = 3
LANES = 128
TAG_ROWS = 8
TQ = 256
TK = 256
SB = 256
WHOLE = 6
NO_TAG = 1 << 30
OUTSIDE = -1e30
MESH = pl.DeviceIdType.MESH
VMEM = pl.BlockSpec(memory_space=pltpu.VMEM)
ANY = pl.BlockSpec(memory_space=pl.ANY)
HBM = pl.BlockSpec(memory_space=pltpu.HBM)


def dot_nt(a, b):
    return lax.dot_general(a, b, (((1,), (1,)), ((), ())), preferred_element_type=jnp.float32)


def dot_nn(a, b):
    return lax.dot_general(a, b, (((1,), (0,)), ((), ())), preferred_element_type=jnp.float32)


def bf16(*shape):
    return jax.ShapeDtypeStruct(shape, jnp.bfloat16)


def f32(*shape):
    return jax.ShapeDtypeStruct(shape, jnp.float32)


def greet(base, pos, team, up, down):
    barrier = pltpu.get_barrier_semaphore()
    for step in range(1, team):
        mate = base + lax.rem(pos + step, team)
        pl.semaphore_signal(barrier, inc=1, device_id=(mate,), device_id_type=MESH)
    pl.semaphore_signal(barrier, inc=1, device_id=(up,), device_id_type=MESH)
    pl.semaphore_signal(barrier, inc=1, device_id=(down,), device_id_type=MESH)
    pl.semaphore_wait(barrier, team + 1)


def place(count, team):
    me = lax.axis_index("img")
    pos = lax.rem(me, team)
    return me, me - pos, pos, lax.rem(me + team, count), lax.rem(me + count - team, count)


def remote(src, dst, send_sem, recv_sem, device):
    return pltpu.make_async_remote_copy(
        src_ref=src, dst_ref=dst, send_sem=send_sem, recv_sem=recv_sem,
        device_id=(device,), device_id_type=MESH)


def lanes_of(pos):
    return pl.ds(pl.multiple_of(pos * LANES, LANES), LANES)


def gather_kernel(count, team, *refs):
    ins, outs = refs[:5], refs[5:10]
    kt, vt, qt, marks = refs[10:14]
    send, recv, halo_send, halo_recv, local = refs[14:]
    tags, kw, vw, _, _ = outs
    me, base, pos, up, down = place(count, team)
    above = me + team < count
    below = me >= team
    greet(base, pos, team, up, down)
    rows = [src.shape[0] for src in ins]
    halos = [REACH * r if t < 3 else 0 for t, r in enumerate(rows)]
    copies, own = [], []
    for t, (src, dst) in enumerate(zip(ins, outs)):
        mine = pl.ds(pl.multiple_of(halos[t] + pos * rows[t], 8), rows[t])
        for step in range(1, team):
            mate = lax.rem(pos + step, team)
            part = src if t == 0 else src.at[:, lanes_of(mate)]
            copy = remote(part, dst.at[mine, :], send.at[t, step], recv.at[t, step], base + mate)
            copy.start()
            copies.append(copy)
        part = src if t == 0 else src.at[:, lanes_of(pos)]
        copy = pltpu.make_async_copy(part, dst.at[mine, :], local.at[t])
        copy.start()
        own.append(copy)

    def halo_copies(t):
        dst, r, h = outs[t], rows[t], halos[t]
        down_copy = remote(dst.at[pl.ds(h, h), :], dst.at[pl.ds(h + team * r, h), :],
                           halo_send.at[t, 0], halo_recv.at[t, 0], down)
        up_copy = remote(dst.at[pl.ds(team * r, h), :], dst.at[pl.ds(0, h), :],
                         halo_send.at[t, 1], halo_recv.at[t, 1], up)
        return down_copy, up_copy

    def arrived(t):
        for copy in copies[t * (team - 1) : (t + 1) * (team - 1)]:
            copy.wait_recv()
        own[t].wait()

    def forward(t):
        down_copy, up_copy = halo_copies(t)
        pl.when(below)(down_copy.start)
        pl.when(above)(up_copy.start)

    def halo_arrived(t):
        down_copy, up_copy = halo_copies(t)
        pl.when(above)(down_copy.wait_recv)
        pl.when(below)(up_copy.wait_recv)

    def flip(src, dst, start, size):
        def step(i, c):
            for u in range(3):
                at = pl.ds(pl.multiple_of(start + (3 * i + u) * LANES, LANES), LANES)
                dst[:, at] = src[at, :].astype(jnp.float32).T.astype(jnp.bfloat16)
            return c
        lax.fori_loop(0, size // LANES // 3, step, 0)

    span = kw.shape[0]
    halo = halos[1]
    inner = span - 2 * halo

    @pl.when(jnp.logical_not(below))
    def _():
        kw[:halo, :] = jnp.zeros((halo, LANES), jnp.bfloat16)
        vw[:halo, :] = jnp.zeros((halo, LANES), jnp.bfloat16)
        used = lax.rem(lax.broadcasted_iota(jnp.int32, (halos[0], LANES), 0), TAG_ROWS)
        tags[: halos[0], :] = jnp.where(used < rows[1] // LANES, 0, NO_TAG)

    @pl.when(jnp.logical_not(above))
    def _():
        kw[halo + inner :, :] = jnp.zeros((halo, LANES), jnp.bfloat16)
        vw[halo + inner :, :] = jnp.zeros((halo, LANES), jnp.bfloat16)
        tags[halos[0] + team * rows[0] :, :] = jnp.full((halos[0], LANES), NO_TAG, jnp.int32)

    arrived(0)
    forward(0)
    arrived(1)
    forward(1)
    halo_arrived(0)
    ids = lax.broadcasted_iota(jnp.int32, (LANES, LANES), 0)

    def mark(i, c):
        for u in range(rows[1] // LANES):
            at = pl.ds(pl.multiple_of(i * rows[1] + u * LANES, LANES), LANES)
            tag = tags[pl.ds(i * TAG_ROWS + u, 1), :]
            outside = (tag <= 0) | (tag >= NO_TAG)
            hit = jnp.where((ids == lax.rem(tag, LANES)) | outside, 1.0, 0.0)
            marks[at, :] = hit.T.astype(jnp.bfloat16)
        return c

    lax.fori_loop(0, span // rows[1], mark, 0)
    flip(kw, kt, halo, inner)
    arrived(2)
    forward(2)
    halo_arrived(1)
    flip(kw, kt, 0, halo)
    flip(kw, kt, halo + inner, halo)
    flip(vw, vt, halo, inner)
    arrived(3)
    flip(outs[3], qt, 0, inner)
    halo_arrived(2)
    flip(vw, vt, 0, halo)
    flip(vw, vt, halo + inner, halo)
    arrived(4)
    for t in range(3):
        down_copy, up_copy = halo_copies(t)
        pl.when(below)(down_copy.wait_send)
        pl.when(above)(up_copy.wait_send)
    for copy in copies:
        copy.wait_send()


def gather(count, team, tags, arrays):
    rows = arrays[0].shape[0]
    span = (team + 2 * REACH) * rows
    return pl.pallas_call(
        lambda *refs: gather_kernel(count, team, *refs),
        out_shape=(
            jax.ShapeDtypeStruct(((team + 2 * REACH) * TAG_ROWS, LANES), jnp.int32),
            bf16(span, LANES), bf16(span, LANES), bf16(team * rows, LANES), bf16(team * rows, LANES),
            bf16(LANES, span), bf16(LANES, span), bf16(LANES, team * rows), bf16(span, LANES)),
        in_specs=[VMEM] * 5,
        out_specs=(VMEM,) * 9,
        scratch_shapes=[
            pltpu.SemaphoreType.DMA((5, team)),
            pltpu.SemaphoreType.DMA((5, team)),
            pltpu.SemaphoreType.DMA((3, 2)),
            pltpu.SemaphoreType.DMA((3, 2)),
            pltpu.SemaphoreType.DMA((5,)),
        ],
        compiler_params=pltpu.CompilerParams(
            collective_id=0, has_side_effects=True, vmem_limit_bytes=16 * 1024 * 1024),
        name="gather",
    )(tags, *arrays)


def attend_kernel(team, rows, *refs):
    tags, kw, vw, qw, gw, kt, vt, qt, marks = refs[:9]
    att_ref, dq_ref, dk_own, dv_own, dk_before, dk_after, dv_before, dv_after = refs[9:17]
    (s_buf, dp_buf, w_buf, p_buf, ds_buf, tops, sums, deltas, dk, dv, att_acc, dq_acc,
     qs, gs, qd, peak, begins, ends) = refs[17:]
    halo = REACH * rows
    own = team * rows
    span = own + 2 * halo
    scale = 1.0 / math.sqrt(HEAD_DIM)
    low = lax.broadcasted_iota(jnp.int32, (TQ, LANES), 1) < HEAD_DIM
    ids = lax.broadcasted_iota(jnp.int32, (LANES, LANES), 0)
    tiles = own // TQ

    def tag_row(row):
        return (row // rows + REACH) * TAG_ROWS + row % rows // LANES

    for tile in range(tiles):
        first = tags[tag_row(tile * TQ) : tag_row(tile * TQ) + 1, :1]
        at = tag_row(tile * TQ + TQ - 1)
        final = tags[at : at + 1, LANES - 1 :]
        every = tags[...]
        begins[tile] = jnp.sum((every < first).astype(jnp.int32))
        ends[tile] = jnp.sum((every <= final).astype(jnp.int32))

    dk[...] = jnp.zeros_like(dk)
    dv[...] = jnp.zeros_like(dv)

    def one_tile(tile, carry):
        row0 = pl.multiple_of(tile * TQ, TQ)
        rows_here = pl.ds(row0, TQ)
        key0 = (begins[tile] // LANES) * LANES
        steps = (ends[tile] - key0 + TK - 1) // TK
        key0 = jnp.minimum(key0, span - steps * TK)

        q = qw[rows_here, :].astype(jnp.float32) * scale
        g = gw[rows_here, :].astype(jnp.float32)
        qd[:TQ, :] = jnp.where(low, q, 0.0).astype(jnp.bfloat16)
        qd[TQ:, :] = jnp.where(low, 0.0, q).astype(jnp.bfloat16)
        gs[:TQ, :] = jnp.where(low, g, 0.0).astype(jnp.bfloat16)
        gs[TQ:, :] = jnp.where(low, 0.0, g).astype(jnp.bfloat16)
        across = (qt[:, rows_here].astype(jnp.float32) * scale).astype(jnp.bfloat16)
        nothing = jnp.zeros((HEAD_DIM, TQ), jnp.bfloat16)
        qs[:HEAD_DIM, :TQ] = across[:HEAD_DIM]
        qs[HEAD_DIM:LANES, :TQ] = nothing
        qs[:HEAD_DIM, TQ:] = nothing
        qs[HEAD_DIM:LANES, TQ:] = across[HEAD_DIM:]
        for u in range(TQ // LANES):
            strip = tile * (TQ // LANES) + u
            per = rows // LANES
            tag = tags[pl.ds((strip // per + REACH) * TAG_ROWS + lax.rem(strip, per), 1), :]
            apart = jnp.where(ids == lax.rem(tag, LANES), 0.0, OUTSIDE).astype(jnp.bfloat16)
            qs[LANES:, u * LANES : (u + 1) * LANES] = apart
            qs[LANES:, TQ + u * LANES : TQ + (u + 1) * LANES] = apart

        def scores(j, many):
            keys = pl.ds(pl.multiple_of(key0 + j * TK, LANES), many * TK)
            here = pl.ds(pl.multiple_of(j * TK, TK), many * TK)
            s_buf[here, :] = dot_nn(jnp.concatenate([kw[keys, :], marks[keys, :]], 1), qs[...])
            dp_buf[here, :] = dot_nt(vw[keys, :], gs[...])

        def weights(j, many):
            for u in range(many * TK // SB):
                here = pl.ds(pl.multiple_of(j * TK + u * SB, SB), SB)
                at = pl.ds(pl.multiple_of(j * (TK // SB * 8) + u * 8, 8), 8)
                s = s_buf[here, :].reshape(SB // 8, 8, 2 * TQ)
                most = jnp.max(s, 0)
                w = jnp.exp(s - most[None])
                w_buf[here, :] = w.reshape(SB, 2 * TQ)
                sums[at, :] = jnp.sum(w, 0)
                deltas[at, :] = jnp.sum(w * dp_buf[here, :].reshape(SB // 8, 8, 2 * TQ), 0)
                tops[at, :] = most
                peak[...] = jnp.maximum(peak[...], most)

        def score(j, many):
            for u in range(many):
                scores(j + u, 1)
                weights(j + u, 1)

        def sweep(body):
            def whole_step(j, c):
                body(WHOLE * j, WHOLE)
                return c

            lax.fori_loop(0, steps // WHOLE, whole_step, 0)
            for rest in range(1, WHOLE):
                @pl.when(lax.rem(steps, WHOLE) == rest)
                def _():
                    body(steps - rest, rest)

        peak[...] = jnp.full((8, 2 * TQ), -3e38, jnp.float32)
        sweep(score)
        parts = steps * (TK // SB)
        top = jnp.max(peak[...], 0, keepdims=True)

        def total_step(j, carry):
            total, delta = carry
            for u in range(TK // SB):
                at = pl.ds(pl.multiple_of(j * (TK // SB * 8) + u * 8, 8), 8)
                factor = jnp.exp(tops[at, :] - top)
                tops[at, :] = factor
                total = total + factor * sums[at, :]
                delta = delta + factor * deltas[at, :]
            return total, delta

        none = jnp.zeros((8, 2 * TQ), jnp.float32)
        total, delta = lax.fori_loop(0, steps, total_step, (none, none))
        inverse = 1.0 / jnp.sum(total, 0, keepdims=True)
        delta = jnp.sum(delta, 0, keepdims=True) * inverse
        att_acc[...] = jnp.zeros_like(att_acc)
        dq_acc[...] = jnp.zeros_like(dq_acc)

        def probs(j, c):
            here = pl.ds(pl.multiple_of(j * SB, SB), SB)
            factor = tops[pl.ds(pl.multiple_of(j * 8, 8), 8), :] * inverse
            p = w_buf[here, :].reshape(SB // 8, 8, 2 * TQ) * factor[None]
            p = p.reshape(SB, 2 * TQ)
            p_buf[here, :] = p.astype(jnp.bfloat16)
            ds_buf[here, :] = (p * (dp_buf[here, :] - delta)).astype(jnp.bfloat16)
            return c

        def grads(j, many):
            keys = pl.ds(pl.multiple_of(key0 + j * TK, LANES), many * TK)
            here = pl.ds(pl.multiple_of(j * TK, TK), many * TK)
            p = p_buf[here, :]
            ds = ds_buf[here, :]
            dk[keys, :] += dot_nn(ds, qd[...])
            dv[keys, :] += dot_nn(p, gs[...])
            for half in (0, 1):
                dims = slice(half * HEAD_DIM, (half + 1) * HEAD_DIM)
                cols = slice(half * TQ, (half + 1) * TQ)
                att_acc[dims, :] += dot_nn(vt[dims, keys], p_buf[here, cols])
                dq_acc[dims, :] += dot_nn(kt[dims, keys], ds_buf[here, cols])

        lax.fori_loop(0, parts, probs, 0)
        sweep(grads)
        att_ref[rows_here, :] = att_acc[...].T.astype(jnp.bfloat16)
        dq_ref[rows_here, :] = (dq_acc[...].T * scale).astype(jnp.bfloat16)
        return carry

    lax.fori_loop(0, tiles, one_tile, 0)
    for acc, mine, before, after in ((dk, dk_own, dk_before, dk_after),
                                     (dv, dv_own, dv_before, dv_after)):
        mine[...] = acc[halo : halo + own, :]
        before[...] = acc[:halo, :].astype(jnp.bfloat16)
        after[...] = acc[halo + own :, :].astype(jnp.bfloat16)


def attend(team, rows, args):
    halo = REACH * rows
    own = team * rows
    span = own + 2 * halo
    held = -(-min(2 * halo + TQ + LANES + TK, span + TK) // TK) * TK
    f = jnp.float32
    scratch = [
        pltpu.VMEM((held, 2 * TQ), f),
        pltpu.VMEM((held, 2 * TQ), f),
        pltpu.VMEM((held, 2 * TQ), f),
        pltpu.VMEM((held, 2 * TQ), jnp.bfloat16),
        pltpu.VMEM((held, 2 * TQ), jnp.bfloat16),
        pltpu.VMEM((held // SB * 8, 2 * TQ), f),
        pltpu.VMEM((held // SB * 8, 2 * TQ), f),
        pltpu.VMEM((held // SB * 8, 2 * TQ), f),
        pltpu.VMEM((span, LANES), f),
        pltpu.VMEM((span, LANES), f),
        pltpu.VMEM((LANES, TQ), f),
        pltpu.VMEM((LANES, TQ), f),
        pltpu.VMEM((2 * LANES, 2 * TQ), jnp.bfloat16),
        pltpu.VMEM((2 * TQ, LANES), jnp.bfloat16),
        pltpu.VMEM((2 * TQ, LANES), jnp.bfloat16),
        pltpu.VMEM((8, 2 * TQ), f),
        pltpu.SMEM((own // TQ,), jnp.int32),
        pltpu.SMEM((own // TQ,), jnp.int32),
    ]
    outs = (bf16(own, LANES), bf16(own, LANES), f32(own, LANES), f32(own, LANES)) + (
        bf16(halo, LANES),) * 4
    return pl.pallas_call(
        lambda *refs: attend_kernel(team, rows, *refs),
        name="attend",
        out_shape=outs,
        in_specs=[VMEM] * len(args),
        out_specs=(VMEM,) * len(outs),
        scratch_shapes=scratch,
        compiler_params=pltpu.CompilerParams(vmem_limit_bytes=35 * 1024 * 1024),
        cost_estimate=pl.CostEstimate(
            flops=60_000_000_000, bytes_accessed=12_000_000, transcendentals=8_000_000),
    )(*args)


def scatter_kernel(count, team, *refs):
    att, dq, dk_own, dv_own, dk_before, dk_after, dv_before, dv_after = refs[:8]
    outs, (above_in, below_in, staged, send, recv, halo_send, halo_recv, local) = refs[8:12], refs[12:]
    me, base, pos, up, down = place(count, team)
    above = me + team < count
    below = me >= team
    rows = outs[0].shape[0]
    halo = REACH * rows
    own = team * rows
    greet(base, pos, team, up, down)

    def halo_copies(t):
        before, after = ((dk_before, dk_after), (dv_before, dv_after))[t]
        return (remote(before, above_in.at[t], halo_send.at[t, 0], halo_recv.at[t, 0], down),
                remote(after, below_in.at[t], halo_send.at[t, 1], halo_recv.at[t, 1], up))

    for t in range(2):
        down_copy, up_copy = halo_copies(t)
        pl.when(below)(down_copy.start)
        pl.when(above)(up_copy.start)
    copies = []

    def spread(t, src):
        for step in range(1, team):
            mate = lax.rem(pos + step, team)
            part = src.at[pl.ds(pl.multiple_of(mate * rows, 16), rows), :]
            copy = remote(part, outs[t].at[:, lanes_of(pos)], send.at[t, step], recv.at[t, step],
                          base + mate)
            copy.start()
            copies.append(copy)
        part = src.at[pl.ds(pl.multiple_of(pos * rows, 16), rows), :]
        copy = pltpu.make_async_copy(part, outs[t].at[:, lanes_of(pos)], local.at[t])
        copy.start()
        return copy

    mine = [spread(0, att), spread(1, dq)]
    for t, src in enumerate((dk_own, dv_own)):
        down_copy, up_copy = halo_copies(t)
        dst = staged.at[t]
        dst[halo : own - halo, :] = src[halo : own - halo, :].astype(jnp.bfloat16)

        @pl.when(above)
        def _():
            down_copy.wait_recv()
            dst[own - halo :, :] = (src[own - halo :, :] + above_in[t].astype(jnp.float32)
                                    ).astype(jnp.bfloat16)

        @pl.when(jnp.logical_not(above))
        def _():
            dst[own - halo :, :] = src[own - halo :, :].astype(jnp.bfloat16)

        @pl.when(below)
        def _():
            up_copy.wait_recv()
            dst[:halo, :] = (src[:halo, :] + below_in[t].astype(jnp.float32)).astype(jnp.bfloat16)

        @pl.when(jnp.logical_not(below))
        def _():
            dst[:halo, :] = src[:halo, :].astype(jnp.bfloat16)

        mine.append(spread(2 + t, dst))
    for copy in mine:
        copy.wait()
    for copy in copies:
        copy.wait_recv()
        copy.wait_send()
    for t in range(2):
        down_copy, up_copy = halo_copies(t)
        pl.when(below)(down_copy.wait_send)
        pl.when(above)(up_copy.wait_send)


def scatter(count, team, rows, arrays):
    halo = REACH * rows
    return pl.pallas_call(
        lambda *refs: scatter_kernel(count, team, *refs),
        out_shape=(bf16(rows, team * LANES),) * 4,
        in_specs=[VMEM] * 8,
        out_specs=(VMEM,) * 4,
        scratch_shapes=[
            pltpu.VMEM((2, halo, LANES), jnp.bfloat16),
            pltpu.VMEM((2, halo, LANES), jnp.bfloat16),
            pltpu.VMEM((2, team * rows, LANES), jnp.bfloat16),
            pltpu.SemaphoreType.DMA((4, team)),
            pltpu.SemaphoreType.DMA((4, team)),
            pltpu.SemaphoreType.DMA((2, 2)),
            pltpu.SemaphoreType.DMA((2, 2)),
            pltpu.SemaphoreType.DMA((4,)),
        ],
        compiler_params=pltpu.CompilerParams(
            collective_id=1, has_side_effects=True, vmem_limit_bytes=20 * 1024 * 1024),
        name="scatter",
    )(*arrays)


def move(arrays, source, target, name, grant):
    def kernel(*refs):
        ins, outs, sems = refs[:4], refs[4:8], refs[8]
        copies = [pltpu.make_async_copy(a, b, sems.at[i]) for i, (a, b) in enumerate(zip(ins, outs))]
        for copy in copies:
            copy.start()
        for copy in copies:
            copy.wait()

    return pl.pallas_call(
        kernel,
        name=name,
        out_shape=tuple(jax.ShapeDtypeStruct(a.shape, a.dtype) for a in arrays),
        in_specs=[source] * 4,
        out_specs=(target,) * 4,
        scratch_shapes=[pltpu.SemaphoreType.DMA((4,))],
        compiler_params=pltpu.CompilerParams(vmem_limit_bytes=grant),
    )(*arrays)


def shards(queries, keys, values, out_grad, image_ids):
    rows, features = queries.shape
    count = lax.axis_size("img")
    team = features // LANES
    tags = jnp.pad((image_ids + 1).reshape(rows // LANES, LANES),
                   ((0, TAG_ROWS - rows // LANES), (0, 0)), constant_values=NO_TAG)
    arrays = move((keys, values, queries, out_grad), HBM, VMEM, "load", 53_200_000)
    gathered = gather(count, team, tags, arrays)
    results = attend(team, rows, gathered)
    attended, query_grad, key_grad, value_grad = scatter(count, team, rows, results)
    return move((attended, query_grad, key_grad, value_grad), VMEM, HBM, "settle", 4 * 1024 * 1024)


def solution(mesh):
    in_specs = (P("img", None), P("img", None), P("img", None), P("img", None), P("img"))
    out_specs = (P("img", None), P("img", None), P("img", None), P("img", None))
    return jax.shard_map(shards, mesh=mesh, in_specs=in_specs, out_specs=out_specs, check_vma=False)
```

```python
import math

import jax
import jax.numpy as jnp
from jax import lax
from jax.experimental import pallas as pl
from jax.experimental.pallas import tpu as pltpu
from jax.sharding import PartitionSpec as P

HEAD_DIM = 64
REACH = 3
LANES = 128
TAG_ROWS = 8
TQ = 256
TK = 256
SB = 256
WHOLE = 6
SLICES = 4
NO_TAG = 1 << 30
OUTSIDE = -1e30
MESH = pl.DeviceIdType.MESH
VMEM = pl.BlockSpec(memory_space=pltpu.VMEM)
ANY = pl.BlockSpec(memory_space=pl.ANY)
HBM = pl.BlockSpec(memory_space=pltpu.HBM)


def dot_nt(a, b):
    return lax.dot_general(a, b, (((1,), (1,)), ((), ())), preferred_element_type=jnp.float32)


def dot_nn(a, b):
    return lax.dot_general(a, b, (((1,), (0,)), ((), ())), preferred_element_type=jnp.float32)


def bf16(*shape):
    return jax.ShapeDtypeStruct(shape, jnp.bfloat16)


def f32(*shape):
    return jax.ShapeDtypeStruct(shape, jnp.float32)


def greet(base, pos, team, up, down):
    barrier = pltpu.get_barrier_semaphore()
    for step in range(1, team):
        mate = base + lax.rem(pos + step, team)
        pl.semaphore_signal(barrier, inc=1, device_id=(mate,), device_id_type=MESH)
    pl.semaphore_signal(barrier, inc=1, device_id=(up,), device_id_type=MESH)
    pl.semaphore_signal(barrier, inc=1, device_id=(down,), device_id_type=MESH)
    pl.semaphore_wait(barrier, team + 1)


def place(count, team):
    me = lax.axis_index("img")
    pos = lax.rem(me, team)
    return me, me - pos, pos, lax.rem(me + team, count), lax.rem(me + count - team, count)


def remote(src, dst, send_sem, recv_sem, device):
    return pltpu.make_async_remote_copy(
        src_ref=src, dst_ref=dst, send_sem=send_sem, recv_sem=recv_sem,
        device_id=(device,), device_id_type=MESH)


def lanes_of(pos):
    return pl.ds(pl.multiple_of(pos * LANES, LANES), LANES)


def gather_kernel(count, team, *refs):
    ins, outs = refs[:5], refs[5:10]
    kt, vt, qt, marks = refs[10:14]
    send, recv, halo_send, halo_recv, local = refs[14:]
    tags, kw, vw, _, _ = outs
    me, base, pos, up, down = place(count, team)
    above = me + team < count
    below = me >= team
    greet(base, pos, team, up, down)
    rows = [src.shape[0] for src in ins]
    halos = [REACH * r if t < 3 else 0 for t, r in enumerate(rows)]
    copies, own = [], []
    for t, (src, dst) in enumerate(zip(ins, outs)):
        mine = pl.ds(pl.multiple_of(halos[t] + pos * rows[t], 8), rows[t])
        for step in range(1, team):
            mate = lax.rem(pos + step, team)
            part = src if t == 0 else src.at[:, lanes_of(mate)]
            copy = remote(part, dst.at[mine, :], send.at[t, step], recv.at[t, step], base + mate)
            copy.start()
            copies.append(copy)
        part = src if t == 0 else src.at[:, lanes_of(pos)]
        copy = pltpu.make_async_copy(part, dst.at[mine, :], local.at[t])
        copy.start()
        own.append(copy)

    def halo_copies(t):
        dst, r, h = outs[t], rows[t], halos[t]
        down_copy = remote(dst.at[pl.ds(h, h), :], dst.at[pl.ds(h + team * r, h), :],
                           halo_send.at[t, 0], halo_recv.at[t, 0], down)
        up_copy = remote(dst.at[pl.ds(team * r, h), :], dst.at[pl.ds(0, h), :],
                         halo_send.at[t, 1], halo_recv.at[t, 1], up)
        return down_copy, up_copy

    def arrived(t):
        for copy in copies[t * (team - 1) : (t + 1) * (team - 1)]:
            copy.wait_recv()
        own[t].wait()

    def forward(t):
        down_copy, up_copy = halo_copies(t)
        pl.when(below)(down_copy.start)
        pl.when(above)(up_copy.start)

    def halo_arrived(t):
        down_copy, up_copy = halo_copies(t)
        pl.when(above)(down_copy.wait_recv)
        pl.when(below)(up_copy.wait_recv)

    def flip(src, dst, start, size):
        def step(i, c):
            for u in range(3):
                at = pl.ds(pl.multiple_of(start + (3 * i + u) * LANES, LANES), LANES)
                dst[:, at] = src[at, :].astype(jnp.float32).T.astype(jnp.bfloat16)
            return c
        lax.fori_loop(0, size // LANES // 3, step, 0)

    span = kw.shape[0]
    halo = halos[1]
    inner = span - 2 * halo

    @pl.when(jnp.logical_not(below))
    def _():
        kw[:halo, :] = jnp.zeros((halo, LANES), jnp.bfloat16)
        vw[:halo, :] = jnp.zeros((halo, LANES), jnp.bfloat16)
        used = lax.rem(lax.broadcasted_iota(jnp.int32, (halos[0], LANES), 0), TAG_ROWS)
        tags[: halos[0], :] = jnp.where(used < rows[1] // LANES, 0, NO_TAG)

    @pl.when(jnp.logical_not(above))
    def _():
        kw[halo + inner :, :] = jnp.zeros((halo, LANES), jnp.bfloat16)
        vw[halo + inner :, :] = jnp.zeros((halo, LANES), jnp.bfloat16)
        tags[halos[0] + team * rows[0] :, :] = jnp.full((halos[0], LANES), NO_TAG, jnp.int32)

    arrived(0)
    forward(0)
    arrived(1)
    forward(1)
    halo_arrived(0)
    ids = lax.broadcasted_iota(jnp.int32, (LANES, LANES), 0)

    def mark(i, c):
        for u in range(rows[1] // LANES):
            at = pl.ds(pl.multiple_of(i * rows[1] + u * LANES, LANES), LANES)
            tag = tags[pl.ds(i * TAG_ROWS + u, 1), :]
            outside = (tag <= 0) | (tag >= NO_TAG)
            hit = jnp.where((ids == lax.rem(tag, LANES)) | outside, 1.0, 0.0)
            marks[at, :] = hit.T.astype(jnp.bfloat16)
        return c

    lax.fori_loop(0, span // rows[1], mark, 0)
    flip(kw, kt, halo, inner)
    arrived(2)
    forward(2)
    halo_arrived(1)
    flip(kw, kt, 0, halo)
    flip(kw, kt, halo + inner, halo)
    flip(vw, vt, halo, inner)
    arrived(3)
    flip(outs[3], qt, 0, inner)
    halo_arrived(2)
    flip(vw, vt, 0, halo)
    flip(vw, vt, halo + inner, halo)
    arrived(4)
    for t in range(3):
        down_copy, up_copy = halo_copies(t)
        pl.when(below)(down_copy.wait_send)
        pl.when(above)(up_copy.wait_send)
    for copy in copies:
        copy.wait_send()


def gather(count, team, tags, arrays):
    rows = arrays[0].shape[0]
    span = (team + 2 * REACH) * rows
    return pl.pallas_call(
        lambda *refs: gather_kernel(count, team, *refs),
        out_shape=(
            jax.ShapeDtypeStruct(((team + 2 * REACH) * TAG_ROWS, LANES), jnp.int32),
            bf16(span, LANES), bf16(span, LANES), bf16(team * rows, LANES), bf16(team * rows, LANES),
            bf16(LANES, span), bf16(LANES, span), bf16(LANES, team * rows), bf16(span, LANES)),
        in_specs=[VMEM] * 5,
        out_specs=(VMEM,) * 9,
        scratch_shapes=[
            pltpu.SemaphoreType.DMA((5, team)),
            pltpu.SemaphoreType.DMA((5, team)),
            pltpu.SemaphoreType.DMA((3, 2)),
            pltpu.SemaphoreType.DMA((3, 2)),
            pltpu.SemaphoreType.DMA((5,)),
        ],
        compiler_params=pltpu.CompilerParams(
            collective_id=0, has_side_effects=True, vmem_limit_bytes=16 * 1024 * 1024),
        name="gather",
    )(tags, *arrays)


def attend_kernel(team, rows, *refs):
    tags, kw, vw, qw, gw, kt, vt, qt, marks = refs[:9]
    att_ref, dq_ref, dk_own, dv_own, dk_before, dk_after, dv_before, dv_after = refs[9:17]
    (s_buf, dp_buf, w_buf, p_buf, ds_buf, tops, sums, deltas, dk, dv, att_acc, dq_acc,
     qs, gs, qd, peak, begins, ends) = refs[17:]
    halo = REACH * rows
    own = team * rows
    span = own + 2 * halo
    scale = 1.0 / math.sqrt(HEAD_DIM)
    low = lax.broadcasted_iota(jnp.int32, (TQ, LANES), 1) < HEAD_DIM
    ids = lax.broadcasted_iota(jnp.int32, (LANES, LANES), 0)
    tiles = own // TQ

    def tag_row(row):
        return (row // rows + REACH) * TAG_ROWS + row % rows // LANES

    for tile in range(tiles):
        first = tags[tag_row(tile * TQ) : tag_row(tile * TQ) + 1, :1]
        at = tag_row(tile * TQ + TQ - 1)
        final = tags[at : at + 1, LANES - 1 :]
        every = tags[...]
        begins[tile] = jnp.sum((every < first).astype(jnp.int32))
        ends[tile] = jnp.sum((every <= final).astype(jnp.int32))

    dk[...] = jnp.zeros_like(dk)
    dv[...] = jnp.zeros_like(dv)

    def one_tile(tile, carry):
        row0 = pl.multiple_of(tile * TQ, TQ)
        rows_here = pl.ds(row0, TQ)
        key0 = (begins[tile] // LANES) * LANES
        steps = (ends[tile] - key0 + TK - 1) // TK
        key0 = jnp.minimum(key0, span - steps * TK)

        q = qw[rows_here, :].astype(jnp.float32) * scale
        g = gw[rows_here, :].astype(jnp.float32)
        qd[:TQ, :] = jnp.where(low, q, 0.0).astype(jnp.bfloat16)
        qd[TQ:, :] = jnp.where(low, 0.0, q).astype(jnp.bfloat16)
        gs[:TQ, :] = jnp.where(low, g, 0.0).astype(jnp.bfloat16)
        gs[TQ:, :] = jnp.where(low, 0.0, g).astype(jnp.bfloat16)
        across = (qt[:, rows_here].astype(jnp.float32) * scale).astype(jnp.bfloat16)
        nothing = jnp.zeros((HEAD_DIM, TQ), jnp.bfloat16)
        qs[:HEAD_DIM, :TQ] = across[:HEAD_DIM]
        qs[HEAD_DIM:LANES, :TQ] = nothing
        qs[:HEAD_DIM, TQ:] = nothing
        qs[HEAD_DIM:LANES, TQ:] = across[HEAD_DIM:]
        for u in range(TQ // LANES):
            strip = tile * (TQ // LANES) + u
            per = rows // LANES
            tag = tags[pl.ds((strip // per + REACH) * TAG_ROWS + lax.rem(strip, per), 1), :]
            apart = jnp.where(ids == lax.rem(tag, LANES), 0.0, OUTSIDE).astype(jnp.bfloat16)
            qs[LANES:, u * LANES : (u + 1) * LANES] = apart
            qs[LANES:, TQ + u * LANES : TQ + (u + 1) * LANES] = apart

        def scores(j, many):
            keys = pl.ds(pl.multiple_of(key0 + j * TK, LANES), many * TK)
            here = pl.ds(pl.multiple_of(j * TK, TK), many * TK)
            s_buf[here, :] = dot_nn(jnp.concatenate([kw[keys, :], marks[keys, :]], 1), qs[...])
            dp_buf[here, :] = dot_nt(vw[keys, :], gs[...])

        def weights(j, many):
            for u in range(many * TK // SB):
                here = pl.ds(pl.multiple_of(j * TK + u * SB, SB), SB)
                at = pl.ds(pl.multiple_of(j * (TK // SB * 8) + u * 8, 8), 8)
                s = s_buf[here, :].reshape(SB // 8, 8, 2 * TQ)
                most = jnp.max(s, 0)
                w = jnp.exp(s - most[None])
                w_buf[here, :] = w.reshape(SB, 2 * TQ)
                sums[at, :] = jnp.sum(w, 0)
                deltas[at, :] = jnp.sum(w * dp_buf[here, :].reshape(SB // 8, 8, 2 * TQ), 0)
                tops[at, :] = most
                peak[...] = jnp.maximum(peak[...], most)

        def score(j, many):
            for u in range(many):
                scores(j + u, 1)
                weights(j + u, 1)

        def sweep(body):
            def whole_step(j, c):
                body(WHOLE * j, WHOLE)
                return c

            lax.fori_loop(0, steps // WHOLE, whole_step, 0)
            for rest in range(1, WHOLE):
                @pl.when(lax.rem(steps, WHOLE) == rest)
                def _():
                    body(steps - rest, rest)

        peak[...] = jnp.full((8, 2 * TQ), -3e38, jnp.float32)
        sweep(score)
        parts = steps * (TK // SB)
        top = jnp.max(peak[...], 0, keepdims=True)

        def total_step(j, carry):
            total, delta = carry
            for u in range(TK // SB):
                at = pl.ds(pl.multiple_of(j * (TK // SB * 8) + u * 8, 8), 8)
                factor = jnp.exp(tops[at, :] - top)
                tops[at, :] = factor
                total = total + factor * sums[at, :]
                delta = delta + factor * deltas[at, :]
            return total, delta

        none = jnp.zeros((8, 2 * TQ), jnp.float32)
        total, delta = lax.fori_loop(0, steps, total_step, (none, none))
        inverse = 1.0 / jnp.sum(total, 0, keepdims=True)
        delta = jnp.sum(delta, 0, keepdims=True) * inverse
        att_acc[...] = jnp.zeros_like(att_acc)
        dq_acc[...] = jnp.zeros_like(dq_acc)

        def probs(j, c):
            here = pl.ds(pl.multiple_of(j * SB, SB), SB)
            factor = tops[pl.ds(pl.multiple_of(j * 8, 8), 8), :] * inverse
            p = w_buf[here, :].reshape(SB // 8, 8, 2 * TQ) * factor[None]
            p = p.reshape(SB, 2 * TQ)
            p_buf[here, :] = p.astype(jnp.bfloat16)
            ds_buf[here, :] = (p * (dp_buf[here, :] - delta)).astype(jnp.bfloat16)
            return c

        def grads(j, many):
            keys = pl.ds(pl.multiple_of(key0 + j * TK, LANES), many * TK)
            here = pl.ds(pl.multiple_of(j * TK, TK), many * TK)
            p = p_buf[here, :]
            ds = ds_buf[here, :]
            dk[keys, :] += dot_nn(ds, qd[...])
            dv[keys, :] += dot_nn(p, gs[...])
            for half in (0, 1):
                dims = slice(half * HEAD_DIM, (half + 1) * HEAD_DIM)
                cols = slice(half * TQ, (half + 1) * TQ)
                att_acc[dims, :] += dot_nn(vt[dims, keys], p_buf[here, cols])
                dq_acc[dims, :] += dot_nn(kt[dims, keys], ds_buf[here, cols])

        lax.fori_loop(0, parts, probs, 0)
        sweep(grads)
        att_ref[rows_here, :] = att_acc[...].T.astype(jnp.bfloat16)
        dq_ref[rows_here, :] = (dq_acc[...].T * scale).astype(jnp.bfloat16)
        return carry

    lax.fori_loop(0, tiles, one_tile, 0)
    for acc, mine, before, after in ((dk, dk_own, dk_before, dk_after),
                                     (dv, dv_own, dv_before, dv_after)):
        mine[...] = acc[halo : halo + own, :]
        before[...] = acc[:halo, :].astype(jnp.bfloat16)
        after[...] = acc[halo + own :, :].astype(jnp.bfloat16)


def attend(team, rows, args):
    halo = REACH * rows
    own = team * rows
    span = own + 2 * halo
    held = -(-min(2 * halo + TQ + LANES + TK, span + TK) // TK) * TK
    f = jnp.float32
    scratch = [
        pltpu.VMEM((held, 2 * TQ), f),
        pltpu.VMEM((held, 2 * TQ), f),
        pltpu.VMEM((held, 2 * TQ), f),
        pltpu.VMEM((held, 2 * TQ), jnp.bfloat16),
        pltpu.VMEM((held, 2 * TQ), jnp.bfloat16),
        pltpu.VMEM((held // SB * 8, 2 * TQ), f),
        pltpu.VMEM((held // SB * 8, 2 * TQ), f),
        pltpu.VMEM((held // SB * 8, 2 * TQ), f),
        pltpu.VMEM((span, LANES), f),
        pltpu.VMEM((span, LANES), f),
        pltpu.VMEM((LANES, TQ), f),
        pltpu.VMEM((LANES, TQ), f),
        pltpu.VMEM((2 * LANES, 2 * TQ), jnp.bfloat16),
        pltpu.VMEM((2 * TQ, LANES), jnp.bfloat16),
        pltpu.VMEM((2 * TQ, LANES), jnp.bfloat16),
        pltpu.VMEM((8, 2 * TQ), f),
        pltpu.SMEM((own // TQ,), jnp.int32),
        pltpu.SMEM((own // TQ,), jnp.int32),
    ]
    outs = (bf16(own, LANES), bf16(own, LANES), f32(own, LANES), f32(own, LANES)) + (
        bf16(halo, LANES),) * 4
    return pl.pallas_call(
        lambda *refs: attend_kernel(team, rows, *refs),
        name="attend",
        out_shape=outs,
        in_specs=[VMEM] * len(args),
        out_specs=(VMEM,) * len(outs),
        scratch_shapes=scratch,
        compiler_params=pltpu.CompilerParams(vmem_limit_bytes=35 * 1024 * 1024),
        cost_estimate=pl.CostEstimate(
            flops=60_000_000_000, bytes_accessed=12_000_000, transcendentals=8_000_000),
    )(*args)


def scatter_kernel(count, team, *refs):
    att, dq, dk_own, dv_own, dk_before, dk_after, dv_before, dv_after = refs[:8]
    outs, (above_in, below_in, staged, send, recv, halo_send, halo_recv, local) = refs[8:12], refs[12:]
    me, base, pos, up, down = place(count, team)
    above = me + team < count
    below = me >= team
    rows = outs[0].shape[0]
    halo = REACH * rows
    own = team * rows
    greet(base, pos, team, up, down)

    def halo_copies(t):
        before, after = ((dk_before, dk_after), (dv_before, dv_after))[t]
        return (remote(before, above_in.at[t], halo_send.at[t, 0], halo_recv.at[t, 0], down),
                remote(after, below_in.at[t], halo_send.at[t, 1], halo_recv.at[t, 1], up))

    for t in range(2):
        down_copy, up_copy = halo_copies(t)
        pl.when(below)(down_copy.start)
        pl.when(above)(up_copy.start)
    copies = []

    def spread(t, src):
        for step in range(1, team):
            mate = lax.rem(pos + step, team)
            part = src.at[pl.ds(pl.multiple_of(mate * rows, 16), rows), :]
            copy = remote(part, outs[t].at[:, lanes_of(pos)], send.at[t, step], recv.at[t, step],
                          base + mate)
            copy.start()
            copies.append(copy)
        part = src.at[pl.ds(pl.multiple_of(pos * rows, 16), rows), :]
        copy = pltpu.make_async_copy(part, outs[t].at[:, lanes_of(pos)], local.at[t])
        copy.start()
        return copy

    mine = [spread(0, att), spread(1, dq)]
    for t, src in enumerate((dk_own, dv_own)):
        down_copy, up_copy = halo_copies(t)
        dst = staged.at[t]
        dst[halo : own - halo, :] = src[halo : own - halo, :].astype(jnp.bfloat16)

        @pl.when(above)
        def _():
            down_copy.wait_recv()
            dst[own - halo :, :] = (src[own - halo :, :] + above_in[t].astype(jnp.float32)
                                    ).astype(jnp.bfloat16)

        @pl.when(jnp.logical_not(above))
        def _():
            dst[own - halo :, :] = src[own - halo :, :].astype(jnp.bfloat16)

        @pl.when(below)
        def _():
            up_copy.wait_recv()
            dst[:halo, :] = (src[:halo, :] + below_in[t].astype(jnp.float32)).astype(jnp.bfloat16)

        @pl.when(jnp.logical_not(below))
        def _():
            dst[:halo, :] = src[:halo, :].astype(jnp.bfloat16)

        mine.append(spread(2 + t, dst))
    for copy in mine:
        copy.wait()
    for copy in copies:
        copy.wait_recv()
        copy.wait_send()
    for t in range(2):
        down_copy, up_copy = halo_copies(t)
        pl.when(below)(down_copy.wait_send)
        pl.when(above)(up_copy.wait_send)


def scatter(count, team, rows, arrays):
    halo = REACH * rows
    return pl.pallas_call(
        lambda *refs: scatter_kernel(count, team, *refs),
        out_shape=(bf16(rows, team * LANES),) * 4,
        in_specs=[VMEM] * 8,
        out_specs=(VMEM,) * 4,
        scratch_shapes=[
            pltpu.VMEM((2, halo, LANES), jnp.bfloat16),
            pltpu.VMEM((2, halo, LANES), jnp.bfloat16),
            pltpu.VMEM((2, team * rows, LANES), jnp.bfloat16),
            pltpu.SemaphoreType.DMA((4, team)),
            pltpu.SemaphoreType.DMA((4, team)),
            pltpu.SemaphoreType.DMA((2, 2)),
            pltpu.SemaphoreType.DMA((2, 2)),
            pltpu.SemaphoreType.DMA((4,)),
        ],
        compiler_params=pltpu.CompilerParams(
            collective_id=1, has_side_effects=True, vmem_limit_bytes=20 * 1024 * 1024),
        name="scatter",
    )(*arrays)


def move(arrays, source, target, name, grant):
    def kernel(*refs):
        ins, outs, sems = refs[:4], refs[4:8], refs[8]
        copies = []
        for i, (a, b) in enumerate(zip(ins, outs)):
            part = a.shape[0] // SLICES
            for j in range(SLICES):
                at = pl.ds(j * part, part)
                copies.append(pltpu.make_async_copy(a.at[at, :], b.at[at, :], sems.at[i, j]))
        for copy in copies:
            copy.start()
        for copy in copies:
            copy.wait()

    return pl.pallas_call(
        kernel,
        name=name,
        out_shape=tuple(jax.ShapeDtypeStruct(a.shape, a.dtype) for a in arrays),
        in_specs=[source] * 4,
        out_specs=(target,) * 4,
        scratch_shapes=[pltpu.SemaphoreType.DMA((4, SLICES))],
        compiler_params=pltpu.CompilerParams(vmem_limit_bytes=grant),
    )(*arrays)


def shards(queries, keys, values, out_grad, image_ids):
    rows, features = queries.shape
    count = lax.axis_size("img")
    team = features // LANES
    tags = jnp.pad((image_ids + 1).reshape(rows // LANES, LANES),
                   ((0, TAG_ROWS - rows // LANES), (0, 0)), constant_values=NO_TAG)
    arrays = move((keys, values, queries, out_grad), HBM, VMEM, "load", 53_200_000)
    gathered = gather(count, team, tags, arrays)
    results = attend(team, rows, gathered)
    attended, query_grad, key_grad, value_grad = scatter(count, team, rows, results)
    return move((attended, query_grad, key_grad, value_grad), VMEM, HBM, "settle", 4 * 1024 * 1024)


def solution(mesh):
    in_specs = (P("img", None), P("img", None), P("img", None), P("img", None), P("img"))
    out_specs = (P("img", None), P("img", None), P("img", None), P("img", None))
    return jax.shard_map(shards, mesh=mesh, in_specs=in_specs, out_specs=out_specs, check_vma=False)
```
